768 devices in a mesh: blk: 384 (over y, x, z), rep: 2 (over core).
Axes of the slice: x: 4, y: 8, z: 12, core: 2. Of those that a mesh axis runs over, the one named last changes fastest.
Arguments:
- star_pos: float32 [3, 98304], P(None, 'blk'), may hold values from -6 to 6
- star_vel: float32 [3, 98304], P(None, 'blk'), may hold values from -3 to 3
- star_acc: float32 [3, 98304], P(None, 'blk'), may hold values from -3 to 3
- star_jerk: float32 [3, 98304], P(None, 'blk'), may hold values from -6 to 6
- masses: float32 [98304], P('blk'), may hold values from 5.086263e-06 to 2.0345053e-05
- act_index: int32 [384, 16], P('blk'), may hold values from 0 to 255, as said below
- act_count: int32 [384], replicated, may hold values from 1 to 16, 3072 in all
Outputs:
- new_pos: float32 [3, 98304], P(None, 'blk')
- new_vel: float32 [3, 98304], P(None, 'blk')
- new_acc: float32 [3, 98304], P(None, 'blk')
- new_jerk: float32 [3, 98304], P(None, 'blk')
The draws below stay inside these ranges and needn't reach their ends.
Inputs may be any that keep to these rules, and one draw needn't show every extreme that they name: `act_index`: within a row all 16 entries differ. `act_count`: the counts sum to 3072, and the largest equals 16.
All inputs are finite; a program needn't handle non-finite values.
Results may differ from the reference program's by a relative error of at most 0.00024.
Values sent between devices are 32-bit elements; how exact they have to be, the bound alone decides.
No kernel may reach another device: no remote copies, remote signals or barrier semaphores. Data moves between devices by JAX's collectives and lax.ppermute only.
A program may use at most 32 MiB of HBM per device.

```python
import math
import jax
import jax.numpy as jnp
import numpy as np
from jax import lax

FLD_DEV = 256
SLOTS = 16
NSTAR = 98304
ACT = 3072
N_BLK = 384


def draw_act_index(key, part):
    row_keys = jax.random.split(jax.random.fold_in(key, 17), N_BLK)

    def one_row(row_key):
        return jax.random.permutation(row_key, FLD_DEV)[:SLOTS]
    return jax.vmap(one_row)(row_keys).astype(jnp.int32)


def levels(stream_key, extent, pieces, smallest, high):
    level = 1.0
    for dim, blocks in pieces:
        draws = jax.random.uniform(jax.random.fold_in(jax.random.fold_in(stream_key, 6), dim), (blocks,), jnp.float32, smallest / len(pieces), high / len(pieces))
        level = level * jnp.repeat(jnp.exp(draws), extent[dim] // blocks).reshape((-1,) + (1,) * (len(extent) - 1 - dim))
    return level


def length_profile(number_of, total, reach, skew):
    loads = [(1 << 20) // math.isqrt(grade ** skew) + 1 for grade in range(2, number_of + 1)]
    rest, holding = total - reach - (number_of - 1), [1] * (number_of - 1)
    while rest > 0:
        candidates = [i for i in range(number_of - 1) if holding[i] < reach]
        pool, budget = sum([loads[i] for i in candidates]), rest
        for i in candidates:
            extra = min(reach - holding[i], max(1, budget * loads[i] // pool), rest)
            holding[i] = holding[i] + extra
            rest = rest - extra
    return np.array([reach] + holding)


def ragged_sizes(rng, amount, total, most, slope):
    if amount == 2:
        one = jax.random.randint(rng, (), max(1, total - most), min(most, total - 1) + 1)
        return jnp.stack([one, total - one])
    sizes = jnp.asarray(length_profile(amount, total, most, slope), jnp.int32)
    twos = (amount - 1) // 2
    giver, sink = sizes[1:1 + 2 * twos:2], sizes[2:2 + 2 * twos:2]
    room = jnp.minimum(giver - 1, most - sink)
    passed = jax.random.randint(jax.random.fold_in(rng, 1), (twos,), 0, 1 << 20) % (room + 1)
    sizes = sizes.at[1:1 + 2 * twos:2].set(giver - passed).at[2:2 + 2 * twos:2].set(sink + passed)
    return sizes[jax.random.permutation(jax.random.fold_in(rng, 2), amount)]


def scatter_about(stream_key, shape, deviation, reach, pieces=(), kind=jnp.bfloat16):
    gain = levels(stream_key, shape, pieces, -0.22, 0.18) if pieces else 1.0
    drawn = jax.random.normal(stream_key, shape, jnp.float32) * deviation * gain
    return jnp.minimum(jnp.maximum(drawn, -reach), reach).astype(kind)


def setup_inputs(seed: int = 0) -> dict:
    key_of = jax.random.split(jax.random.key(seed), 8)
    star_pos = scatter_about(key_of[0], (3, NSTAR), 1.0, 6.0, ((1, 384),), jnp.float32)
    star_vel = scatter_about(key_of[1], (3, NSTAR), 0.5, 3.0, ((1, 384),), jnp.float32)
    star_acc = scatter_about(key_of[2], (3, NSTAR), 0.5, 3.0, ((1, 384),), jnp.float32)
    star_jerk = scatter_about(key_of[3], (3, NSTAR), 1.0, 6.0, ((1, 384),), jnp.float32)
    masses = jnp.clip(jnp.exp(math.log(2.0345052689663135e-05) - 1.3862944 * jax.random.uniform(key_of[4], (NSTAR,), jnp.float32) ** levels(key_of[4], (NSTAR,), ((0, 384),), -0.2, 0.2)), 5.086263172415784e-06, 2.0345052689663135e-05)
    act_index = draw_act_index(jax.random.fold_in(key_of[7], 71), 0)
    act_count = ragged_sizes(key_of[6], N_BLK, ACT, SLOTS, 2).astype(jnp.int32)
    return {"star_pos": star_pos, "star_vel": star_vel, "star_acc": star_acc, "star_jerk": star_jerk, "masses": masses, "act_index": act_index, "act_count": act_count}


STEP_TIME = 0.0625
SOFTEN_SQ = 0.0001

def predict(position, velocity, accel, jerk_old):
    half_sq = STEP_TIME * STEP_TIME / 2.0
    pred_pos = position + STEP_TIME * velocity + half_sq * accel + STEP_TIME * half_sq / 3.0 * jerk_old
    pred_vel = velocity + STEP_TIME * accel + half_sq * jerk_old
    return (pred_pos, pred_vel)

def pair_forces(active, field, tile_cap):
    count_cols = active.shape[1]
    tile_width = tile_cap
    while count_cols % tile_width != 0:
        tile_width = tile_width // 2
    blocks = active.reshape(6, count_cols // tile_width, tile_width).transpose(1, 0, 2)

    def one_block(block):
        delta_x = field[0][None, :] - block[0][:, None]
        delta_y = field[1][None, :] - block[1][:, None]
        delta_z = field[2][None, :] - block[2][:, None]
        delta_u = field[3][None, :] - block[3][:, None]
        delta_v = field[4][None, :] - block[4][:, None]
        delta_w = field[5][None, :] - block[5][:, None]
        radius_sq = delta_x * delta_x + delta_y * delta_y + delta_z * delta_z + SOFTEN_SQ
        inverse = 1.0 / radius_sq
        weight = field[6][None, :] * inverse * jnp.sqrt(inverse)
        radial = 3.0 * (delta_x * delta_u + delta_y * delta_v + delta_z * delta_w) * inverse
        return jnp.stack([lax.optimization_barrier(jnp.sum(weight * delta_x, axis=1)), lax.optimization_barrier(jnp.sum(weight * delta_y, axis=1)), lax.optimization_barrier(jnp.sum(weight * delta_z, axis=1)), lax.optimization_barrier(jnp.sum(weight * (delta_u - radial * delta_x), axis=1)), lax.optimization_barrier(jnp.sum(weight * (delta_v - radial * delta_y), axis=1)), lax.optimization_barrier(jnp.sum(weight * (delta_w - radial * delta_z), axis=1))])
    result = lax.map(one_block, blocks)
    return result.transpose(1, 0, 2).reshape(6, count_cols)

def correct(state_old, forces):
    pos_zero = state_old[0:3]
    vel_zero = state_old[3:6]
    acc_zero = state_old[6:9]
    jerk_zero = state_old[9:12]
    acc_one = forces[0:3]
    jerk_one = forces[3:6]
    vel_one = vel_zero + (acc_zero + acc_one) * (STEP_TIME / 2.0) + (jerk_zero - jerk_one) * (STEP_TIME * STEP_TIME / 12.0)
    pos_one = pos_zero + (vel_zero + vel_one) * (STEP_TIME / 2.0) + (acc_zero - acc_one) * (STEP_TIME * STEP_TIME / 12.0)
    return jnp.concatenate([pos_one, vel_one, acc_one, jerk_one], axis=0)

def reference(star_pos, star_vel, star_acc, star_jerk, masses, act_index, act_count):
    pred_pos, pred_vel = predict(star_pos, star_vel, star_acc, star_jerk)
    field = jnp.concatenate([pred_pos, pred_vel, masses[None, :]], axis=0)
    ends = jnp.cumsum(act_count).astype(jnp.int32)
    starts = (ends - act_count).astype(jnp.int32)
    ranks = jnp.arange(ACT, dtype=jnp.int32)
    shard_of = jnp.searchsorted(ends, ranks, side='right').astype(jnp.int32)
    slot_of = (ranks - starts[shard_of]).astype(jnp.int32)
    global_idx = (shard_of * FLD_DEV + act_index[shard_of, slot_of]).astype(jnp.int32)
    forces = pair_forces(field[0:6][:, global_idx], field, 64)
    state = jnp.concatenate([star_pos, star_vel, star_acc, star_jerk], axis=0)
    updated = correct(state[:, global_idx], forces)
    state = state.at[:, global_idx].set(updated)
    return (state[0:3], state[3:6], state[6:9], state[9:12])
```

```python
import jax
import jax.numpy as jnp
from jax import lax
from jax.experimental import pallas as pl
from jax.experimental.pallas import tpu as pltpu
from jax.sharding import Mesh
from jax.sharding import PartitionSpec as P

Y, X, Z, REP = "blk_0", "blk_1", "blk_2", "rep"
BLK = (Y, X, Z)
FIELD_AXES = (Y, X)
ACT_AXIS = Z

STEP_TIME = 0.0625
SOFTEN_SQ = 0.0001
HALF_SQ = STEP_TIME * STEP_TIME / 2.0
LANES = 128
SLOTS = 16
WIDE = 256
LIMIT = 8 * 1024 * 1024
EXACT = lax.Precision.HIGHEST


def lane_iota(shape):
    return lax.broadcasted_iota(jnp.int32, shape, len(shape) - 1)


def row_iota(shape):
    return lax.broadcasted_iota(jnp.int32, shape, len(shape) - 2)


def tiled_slots(index_ref, scratch):
    scratch[...] = jnp.zeros(scratch.shape, jnp.int32)
    scratch[0:1, 0:SLOTS] = index_ref[...]
    row = scratch[0:1, :]
    for shift in (16, 32, 64):
        row = row + pltpu.roll(row, shift, 1)
    return row


def own_rows(shape):
    return row_iota(shape) == lane_iota(shape) // SLOTS


def prepare_kernel(pos, vel, acc, jerk, mass, index, field_out, act_out, state, slots):
    cubed = STEP_TIME * HALF_SQ / 3.0
    state[0:3, :] = pos[...] + STEP_TIME * vel[...] + HALF_SQ * acc[...] + cubed * jerk[...]
    state[3:6, :] = vel[...] + STEP_TIME * acc[...] + HALF_SQ * jerk[...]
    state[6:7, :] = mass[...]
    state[7:8, :] = jnp.zeros((1, state.shape[1]), jnp.float32)
    whole = state[...]
    half = jnp.where(lax.axis_index(REP) == 0, whole[:, :LANES], whole[:, LANES:])
    for k in range(field_out.shape[0]):
        field_out[k] = half
    shape = (whole.shape[1], LANES)
    chosen = (row_iota(shape) == tiled_slots(index, slots)).astype(jnp.float32)
    picked = jnp.dot(whole, chosen, precision=EXACT, preferred_element_type=jnp.float32)
    packed = jnp.sum(jnp.where(own_rows(picked.shape), picked, 0.0), axis=0, keepdims=True)
    for k in range(act_out.shape[0]):
        act_out[k] = packed


def line_base():
    y, x, z = lax.axis_index(Y), lax.axis_index(X), lax.axis_index(Z)
    return y, x, z


def forces_kernel(line, count, field, act, out, rows, active, sums):
    n_line = act.shape[0]
    n_field = field.shape[0]
    first, stride = line()
    rows[...] = jnp.zeros(rows.shape, jnp.float32)
    for k in range(n_line):
        rows[k : k + 1, :] = act[k]
    columns = rows[...].T
    starts = []
    lives = []
    total = 0
    for k in range(n_line):
        live = count[first + k * stride]
        starts.append(total)
        lives.append(live)
        total = total + live
    for k in range(n_line):
        spread = jnp.broadcast_to(columns[0:96, k : k + 1], (96, LANES))
        for c in range(6):
            active[c, pl.ds(starts[k], SLOTS), :] = spread[c * SLOTS : (c + 1) * SLOTS]

    def one_block(b, carry):
        at = pl.ds(pl.multiple_of(b * 8, 8), 8)
        mine = [active[c, at, :] for c in range(6)]

        def one_chunk(f, sums_here):
            def row(c):
                return jnp.broadcast_to(field[f, c : c + 1, :], (8, LANES))

            dx, dy, dz, du, dv, dw = [row(c) - mine[c] for c in range(6)]
            radius_sq = dx * dx + dy * dy + dz * dz + SOFTEN_SQ
            root = lax.rsqrt(radius_sq)
            inverse = root * root
            weight = row(6) * root * inverse
            radial = (dx * du + dy * dv + dz * dw) * inverse
            wx, wy, wz = weight * dx, weight * dy, weight * dz
            new = (wx, wy, wz, weight * du, weight * dv, weight * dw, radial * wx, radial * wy, radial * wz)
            return tuple(s + n for s, n in zip(sums_here, new))

        zero = jnp.zeros((8, LANES), jnp.float32)
        got = lax.fori_loop(0, n_field, one_chunk, (zero,) * 9, unroll=4)
        for c in range(3):
            sums[c, at, :] = got[c]
            sums[3 + c, at, :] = got[3 + c] - 3.0 * got[6 + c]
        return carry

    lax.fori_loop(0, (total + 7) // 8, one_block, 0)
    folded = jnp.zeros((8, WIDE), jnp.float32)
    for c in range(6):
        ones = (row_iota((8, LANES)) == c).astype(jnp.float32)
        row = lax.dot_general(
            ones, sums[c], (((1,), (1,)), ((), ())), precision=EXACT, preferred_element_type=jnp.float32
        )
        row = jnp.where(row_iota((8, WIDE)) == c, row, 0.0)
        folded = folded + (pltpu.roll(row, SLOTS * c, 1) if c else row)
    lane = lane_iota((8, LANES))
    owned = own_rows((8, LANES))
    for k in range(n_line):
        moved = (pltpu.roll(folded, WIDE - starts[k], 1) if k else folded)[:, :LANES]
        kept = jnp.where(owned & (lane % SLOTS < lives[k]), moved, 0.0)
        packed = jnp.sum(kept, axis=0, keepdims=True)
        out[2 * k] = packed
        out[2 * k + 1] = packed


def correct_kernel(count, parts, pos, vel, acc, jerk, index, new_pos, new_vel, new_acc, new_jerk, slots):
    y, x, z = line_base()
    live = count[(y * lax.axis_size(X) + x) * lax.axis_size(Z) + z]
    force = parts[0]
    for k in range(1, parts.shape[0]):
        force = force + parts[k]
    shape = (8, LANES)
    lane = lane_iota(shape)
    spread = jnp.where(own_rows(shape), jnp.broadcast_to(force, shape), 0.0)
    spread = jnp.where((row_iota(shape) == 6) & own_rows(shape), 1.0, spread)
    table = (pos.shape[1], LANES)
    chosen = (row_iota(table) == tiled_slots(index, slots)) & (lane_iota(table) % SLOTS < live)
    placed = lax.dot_general(
        spread, chosen.astype(jnp.float32), (((1,), (1,)), ((), ())), precision=EXACT, preferred_element_type=jnp.float32
    )
    hit = jnp.broadcast_to(placed[6:7], (3, placed.shape[1])) > 0.5
    acc_one, jerk_one = placed[0:3], placed[3:6]
    pos_zero, vel_zero, acc_zero, jerk_zero = pos[...], vel[...], acc[...], jerk[...]
    twelfth = STEP_TIME * STEP_TIME / 12.0
    vel_one = vel_zero + (acc_zero + acc_one) * (STEP_TIME / 2.0) + (jerk_zero - jerk_one) * twelfth
    pos_one = pos_zero + (vel_zero + vel_one) * (STEP_TIME / 2.0) + (acc_zero - acc_one) * twelfth
    new_pos[...] = jnp.where(hit, pos_one, pos_zero)
    new_vel[...] = jnp.where(hit, vel_one, vel_zero)
    new_acc[...] = jnp.where(hit, acc_one, acc_zero)
    new_jerk[...] = jnp.where(hit, jerk_one, jerk_zero)


def f32(*shape):
    return jax.ShapeDtypeStruct(shape, jnp.float32)


VMEM = pl.BlockSpec(memory_space=pltpu.VMEM)
SMEM = pl.BlockSpec(memory_space=pltpu.SMEM)


def shards(star_pos, star_vel, star_acc, star_jerk, masses, act_index, act_count):
    n_field = lax.axis_size(FIELD_AXES)
    n_line = lax.axis_size(ACT_AXIS)
    state = (star_pos, star_vel, star_acc, star_jerk)
    width = star_pos.shape[1]

    def line():
        y, x, z = line_base()
        return (y * lax.axis_size(X) + x) * lax.axis_size(Z), 1

    field, act = pl.pallas_call(
        prepare_kernel,
        out_shape=(f32(n_field, 8, LANES), f32(n_line, 1, LANES)),
        in_specs=[VMEM] * 6,
        out_specs=(VMEM, VMEM),
        scratch_shapes=[pltpu.VMEM((8, width), jnp.float32), pltpu.VMEM((8, LANES), jnp.int32)],
        compiler_params=pltpu.CompilerParams(vmem_limit_bytes=LIMIT),
        name="prepare",
    )(*state, masses[None, :], act_index)
    act = lax.all_to_all(act, ACT_AXIS, 0, 0, tiled=True)
    field = lax.all_to_all(field, FIELD_AXES, 0, 0, tiled=True)
    parts = pl.pallas_call(
        lambda *refs: forces_kernel(line, *refs),
        out_shape=f32(2 * n_line, 1, LANES),
        in_specs=[SMEM, VMEM, VMEM],
        out_specs=VMEM,
        scratch_shapes=[
            pltpu.VMEM((16, LANES), jnp.float32),
            pltpu.VMEM((6, WIDE, LANES), jnp.float32),
            pltpu.VMEM((6, WIDE, LANES), jnp.float32),
        ],
        compiler_params=pltpu.CompilerParams(vmem_limit_bytes=LIMIT),
        name="forces",
    )(act_count, field, act)
    parts = lax.all_to_all(parts, (ACT_AXIS, REP), 0, 0, tiled=True)
    return pl.pallas_call(
        correct_kernel,
        out_shape=tuple(f32(3, width) for _ in range(4)),
        in_specs=[SMEM] + [VMEM] * 6,
        out_specs=(VMEM,) * 4,
        scratch_shapes=[pltpu.VMEM((8, LANES), jnp.int32)],
        compiler_params=pltpu.CompilerParams(vmem_limit_bytes=LIMIT),
        name="correct",
    )(act_count, parts, *state, act_index)


def solution(mesh):
    finer = Mesh(mesh.devices.reshape(8, 4, 12, mesh.shape["rep"]), (Y, X, Z, REP))
    placed = (P(None, BLK), P(None, BLK), P(None, BLK), P(None, BLK), P(BLK), P(BLK, None), P())
    return jax.shard_map(
        shards,
        mesh=finer,
        in_specs=placed,
        out_specs=(P(None, BLK), P(None, BLK), P(None, BLK), P(None, BLK)),
        check_vma=False,
    )
```

```python
import jax
import jax.numpy as jnp
from jax import lax
from jax.experimental import pallas as pl
from jax.experimental.pallas import tpu as pltpu
from jax.sharding import Mesh
from jax.sharding import PartitionSpec as P

Y, X, Z, REP = "blk_0", "blk_1", "blk_2", "rep"
BLK = (Y, X, Z)
FIELD_AXES = (X, Z)
ACT_AXIS = Y

STEP_TIME = 0.0625
SOFTEN_SQ = 0.0001
HALF_SQ = STEP_TIME * STEP_TIME / 2.0
LANES = 128
SLOTS = 16
WIDE = 256
LIMIT = 8 * 1024 * 1024
EXACT = lax.Precision.HIGHEST


def lane_iota(shape):
    return lax.broadcasted_iota(jnp.int32, shape, len(shape) - 1)


def row_iota(shape):
    return lax.broadcasted_iota(jnp.int32, shape, len(shape) - 2)


def tiled_slots(index_ref, scratch):
    scratch[...] = jnp.zeros(scratch.shape, jnp.int32)
    scratch[0:1, 0:SLOTS] = index_ref[...]
    row = scratch[0:1, :]
    for shift in (16, 32, 64):
        row = row + pltpu.roll(row, shift, 1)
    return row


def own_rows(shape):
    return row_iota(shape) == lane_iota(shape) // SLOTS


def prepare_kernel(*refs):
    given, (field_out, act_out), (pos, vel, acc, jerk, mass, index, state, slots, done) = refs[:6], refs[6:8], refs[8:]
    copies = [
        pltpu.make_async_copy(far, near, done.at[k])
        for k, (far, near) in enumerate(zip(given, (pos, vel, acc, jerk, mass, index)))
    ]
    for copy in copies:
        copy.start()
    for copy in copies:
        copy.wait()
    cubed = STEP_TIME * HALF_SQ / 3.0
    state[0:3, :] = pos[...] + STEP_TIME * vel[...] + HALF_SQ * acc[...] + cubed * jerk[...]
    state[3:6, :] = vel[...] + STEP_TIME * acc[...] + HALF_SQ * jerk[...]
    state[6:7, :] = mass[...]
    state[7:8, :] = jnp.zeros((1, state.shape[1]), jnp.float32)
    whole = state[...]
    half = jnp.where(lax.axis_index(REP) == 0, whole[:, :LANES], whole[:, LANES:])
    for k in range(field_out.shape[0]):
        field_out[k] = half
    shape = (whole.shape[1], LANES)
    chosen = (row_iota(shape) == tiled_slots(index, slots)).astype(jnp.float32)
    picked = jnp.dot(whole, chosen, precision=EXACT, preferred_element_type=jnp.float32)
    packed = jnp.sum(jnp.where(own_rows(picked.shape), picked, 0.0), axis=0, keepdims=True)
    for k in range(act_out.shape[0]):
        act_out[k] = packed


def line_base():
    y, x, z = lax.axis_index(Y), lax.axis_index(X), lax.axis_index(Z)
    return y, x, z


def forces_kernel(line, count, field, act, out, rows, active, sums):
    n_line = act.shape[0]
    n_field = field.shape[0]
    first, stride = line()
    rows[...] = jnp.zeros(rows.shape, jnp.float32)
    for k in range(n_line):
        rows[k : k + 1, :] = act[k]
    columns = rows[...].T
    starts = []
    lives = []
    total = 0
    for k in range(n_line):
        live = count[first + k * stride]
        starts.append(total)
        lives.append(live)
        total = total + live
    for k in range(n_line):
        spread = jnp.broadcast_to(columns[0:96, k : k + 1], (96, LANES))
        for c in range(6):
            active[c, pl.ds(starts[k], SLOTS), :] = spread[c * SLOTS : (c + 1) * SLOTS]

    def one_block(b, carry):
        at = pl.ds(pl.multiple_of(b * 8, 8), 8)
        mine = [active[c, at, :] for c in range(6)]

        def one_chunk(f, sums_here):
            def row(c):
                return jnp.broadcast_to(field[f, c : c + 1, :], (8, LANES))

            dx, dy, dz, du, dv, dw = [row(c) - mine[c] for c in range(6)]
            radius_sq = dx * dx + dy * dy + dz * dz + SOFTEN_SQ
            root = lax.rsqrt(radius_sq)
            inverse = root * root
            weight = row(6) * root * inverse
            radial = (dx * du + dy * dv + dz * dw) * inverse
            wx, wy, wz = weight * dx, weight * dy, weight * dz
            new = (wx, wy, wz, weight * du, weight * dv, weight * dw, radial * wx, radial * wy, radial * wz)
            return tuple(s + n for s, n in zip(sums_here, new))

        zero = jnp.zeros((8, LANES), jnp.float32)
        got = lax.fori_loop(0, n_field, one_chunk, (zero,) * 9, unroll=4)
        for c in range(3):
            sums[c, at, :] = got[c]
            sums[3 + c, at, :] = got[3 + c] - 3.0 * got[6 + c]
        return carry

    lax.fori_loop(0, (total + 7) // 8, one_block, 0)
    folded = jnp.zeros((8, WIDE), jnp.float32)
    for c in range(6):
        ones = (row_iota((8, LANES)) == c).astype(jnp.float32)
        row = lax.dot_general(
            ones, sums[c], (((1,), (1,)), ((), ())), precision=EXACT, preferred_element_type=jnp.float32
        )
        row = jnp.where(row_iota((8, WIDE)) == c, row, 0.0)
        folded = folded + (pltpu.roll(row, SLOTS * c, 1) if c else row)
    lane = lane_iota((8, LANES))
    owned = own_rows((8, LANES))
    for k in range(n_line):
        moved = (pltpu.roll(folded, WIDE - starts[k], 1) if k else folded)[:, :LANES]
        kept = jnp.where(owned & (lane % SLOTS < lives[k]), moved, 0.0)
        packed = jnp.sum(kept, axis=0, keepdims=True)
        out[2 * k] = packed
        out[2 * k + 1] = packed


def correct_kernel(count, parts, pos, vel, acc, jerk, index, new_pos, new_vel, new_acc, new_jerk, slots):
    y, x, z = line_base()
    live = count[(y * lax.axis_size(X) + x) * lax.axis_size(Z) + z]
    force = parts[0]
    for k in range(1, parts.shape[0]):
        force = force + parts[k]
    shape = (8, LANES)
    lane = lane_iota(shape)
    spread = jnp.where(own_rows(shape), jnp.broadcast_to(force, shape), 0.0)
    spread = jnp.where((row_iota(shape) == 6) & own_rows(shape), 1.0, spread)
    table = (pos.shape[1], LANES)
    chosen = (row_iota(table) == tiled_slots(index, slots)) & (lane_iota(table) % SLOTS < live)
    placed = lax.dot_general(
        spread, chosen.astype(jnp.float32), (((1,), (1,)), ((), ())), precision=EXACT, preferred_element_type=jnp.float32
    )
    hit = jnp.broadcast_to(placed[6:7], (3, placed.shape[1])) > 0.5
    acc_one, jerk_one = placed[0:3], placed[3:6]
    pos_zero, vel_zero, acc_zero, jerk_zero = pos[...], vel[...], acc[...], jerk[...]
    twelfth = STEP_TIME * STEP_TIME / 12.0
    vel_one = vel_zero + (acc_zero + acc_one) * (STEP_TIME / 2.0) + (jerk_zero - jerk_one) * twelfth
    pos_one = pos_zero + (vel_zero + vel_one) * (STEP_TIME / 2.0) + (acc_zero - acc_one) * twelfth
    new_pos[...] = jnp.where(hit, pos_one, pos_zero)
    new_vel[...] = jnp.where(hit, vel_one, vel_zero)
    new_acc[...] = jnp.where(hit, acc_one, acc_zero)
    new_jerk[...] = jnp.where(hit, jerk_one, jerk_zero)


def f32(*shape):
    return jax.ShapeDtypeStruct(shape, jnp.float32)


VMEM = pl.BlockSpec(memory_space=pltpu.VMEM)
HBM = pl.BlockSpec(memory_space=pltpu.HBM)
SMEM = pl.BlockSpec(memory_space=pltpu.SMEM)


def shards(star_pos, star_vel, star_acc, star_jerk, masses, act_index, act_count):
    n_field = lax.axis_size(FIELD_AXES)
    n_line = lax.axis_size(ACT_AXIS)
    state = (star_pos, star_vel, star_acc, star_jerk)
    width = star_pos.shape[1]

    def line():
        y, x, z = line_base()
        return x * lax.axis_size(Z) + z, lax.axis_size(X) * lax.axis_size(Z)

    field, act = pl.pallas_call(
        prepare_kernel,
        out_shape=(f32(n_field, 8, LANES), f32(n_line, 1, LANES)),
        in_specs=[HBM] * 6,
        out_specs=(VMEM, VMEM),
        scratch_shapes=[pltpu.VMEM((3, width), jnp.float32)] * 4
        + [
            pltpu.VMEM((1, width), jnp.float32),
            pltpu.VMEM((1, SLOTS), jnp.int32),
            pltpu.VMEM((8, width), jnp.float32),
            pltpu.VMEM((8, LANES), jnp.int32),
            pltpu.SemaphoreType.DMA((6,)),
        ],
        compiler_params=pltpu.CompilerParams(vmem_limit_bytes=LIMIT),
        name="prepare",
    )(*state, masses[None, :], act_index)
    act = lax.all_to_all(act, ACT_AXIS, 0, 0, tiled=True)
    field = lax.all_to_all(field, FIELD_AXES, 0, 0, tiled=True)
    parts = pl.pallas_call(
        lambda *refs: forces_kernel(line, *refs),
        out_shape=f32(2 * n_line, 1, LANES),
        in_specs=[SMEM, VMEM, VMEM],
        out_specs=VMEM,
        scratch_shapes=[
            pltpu.VMEM((16, LANES), jnp.float32),
            pltpu.VMEM((6, WIDE, LANES), jnp.float32),
            pltpu.VMEM((6, WIDE, LANES), jnp.float32),
        ],
        compiler_params=pltpu.CompilerParams(vmem_limit_bytes=LIMIT),
        name="forces",
    )(act_count, field, act)
    parts = lax.all_to_all(parts, (ACT_AXIS, REP), 0, 0, tiled=True)
    return pl.pallas_call(
        correct_kernel,
        out_shape=tuple(f32(3, width) for _ in range(4)),
        in_specs=[SMEM] + [VMEM] * 6,
        out_specs=(VMEM,) * 4,
        scratch_shapes=[pltpu.VMEM((8, LANES), jnp.int32)],
        compiler_params=pltpu.CompilerParams(vmem_limit_bytes=LIMIT),
        name="correct",
    )(act_count, parts, *state, act_index)


def solution(mesh):
    finer = Mesh(mesh.devices.reshape(8, 4, 12, mesh.shape["rep"]), (Y, X, Z, REP))
    placed = (P(None, BLK), P(None, BLK), P(None, BLK), P(None, BLK), P(BLK), P(BLK, None), P())
    return jax.shard_map(
        shards,
        mesh=finer,
        in_specs=placed,
        out_specs=(P(None, BLK), P(None, BLK), P(None, BLK), P(None, BLK)),
        check_vma=False,
    )
```

```python
import jax
import jax.numpy as jnp
from jax import lax
from jax.experimental import pallas as pl
from jax.experimental.pallas import tpu as pltpu
from jax.sharding import Mesh
from jax.sharding import PartitionSpec as P

Y, X, Z, REP = "blk_0", "blk_1", "blk_2", "rep"
BLK = (Y, X, Z)
FIELD_AXES = (X, Z)
ACT_AXIS = Y

STEP_TIME = 0.0625
SOFTEN_SQ = 0.0001
HALF_SQ = STEP_TIME * STEP_TIME / 2.0
LANES = 128
SLOTS = 16
WIDE = 256
LIMIT = 8 * 1024 * 1024
EXACT = lax.Precision.HIGHEST


def lane_iota(shape):
    return lax.broadcasted_iota(jnp.int32, shape, len(shape) - 1)


def row_iota(shape):
    return lax.broadcasted_iota(jnp.int32, shape, len(shape) - 2)


def tiled_slots(index_ref, scratch):
    scratch[...] = jnp.zeros(scratch.shape, jnp.int32)
    scratch[0:1, 0:SLOTS] = index_ref[...]
    row = scratch[0:1, :]
    for shift in (16, 32, 64):
        row = row + pltpu.roll(row, shift, 1)
    return row


def own_rows(shape):
    return row_iota(shape) == lane_iota(shape) // SLOTS


def prepare_kernel(*refs):
    given, (field_out, act_out), (pos, vel, acc, jerk, mass, index, state, slots, done) = refs[:6], refs[6:8], refs[8:]
    copies = [
        pltpu.make_async_copy(far, near, done.at[k])
        for k, (far, near) in enumerate(zip(given, (pos, vel, acc, jerk, mass, index)))
    ]
    for copy in copies:
        copy.start()
    for copy in copies:
        copy.wait()
    cubed = STEP_TIME * HALF_SQ / 3.0
    state[0:3, :] = pos[...] + STEP_TIME * vel[...] + HALF_SQ * acc[...] + cubed * jerk[...]
    state[3:6, :] = vel[...] + STEP_TIME * acc[...] + HALF_SQ * jerk[...]
    state[6:7, :] = mass[...]
    state[7:8, :] = jnp.zeros((1, state.shape[1]), jnp.float32)
    whole = state[...]
    half = jnp.where(lax.axis_index(REP) == 0, whole[:, :LANES], whole[:, LANES:])
    for k in range(field_out.shape[0]):
        field_out[k] = half
    shape = (whole.shape[1], LANES)
    chosen = (row_iota(shape) == tiled_slots(index, slots)).astype(jnp.float32)
    picked = jnp.dot(whole, chosen, precision=EXACT, preferred_element_type=jnp.float32)
    packed = jnp.sum(jnp.where(own_rows(picked.shape), picked, 0.0), axis=0, keepdims=True)
    act_out[...] = packed


def line_base():
    y, x, z = lax.axis_index(Y), lax.axis_index(X), lax.axis_index(Z)
    return y, x, z


def forces_kernel(line, count, field, act, out, rows, active, sums):
    n_line = act.shape[0]
    n_field = field.shape[0]
    first, stride = line()
    rows[...] = jnp.zeros(rows.shape, jnp.float32)
    for k in range(n_line):
        rows[k : k + 1, :] = act[k]
    columns = rows[...].T
    starts = []
    lives = []
    total = 0
    for k in range(n_line):
        live = count[first + k * stride]
        starts.append(total)
        lives.append(live)
        total = total + live
    for k in range(n_line):
        spread = jnp.broadcast_to(columns[0:96, k : k + 1], (96, LANES))
        for c in range(6):
            active[c, pl.ds(starts[k], SLOTS), :] = spread[c * SLOTS : (c + 1) * SLOTS]

    def one_block(b, carry):
        at = pl.ds(pl.multiple_of(b * 8, 8), 8)
        mine = [active[c, at, :] for c in range(6)]

        def one_chunk(f, sums_here):
            def row(c):
                return jnp.broadcast_to(field[f, c : c + 1, :], (8, LANES))

            dx, dy, dz, du, dv, dw = [row(c) - mine[c] for c in range(6)]
            radius_sq = dx * dx + dy * dy + dz * dz + SOFTEN_SQ
            root = lax.rsqrt(radius_sq)
            inverse = root * root
            weight = row(6) * root * inverse
            radial = (dx * du + dy * dv + dz * dw) * inverse
            wx, wy, wz = weight * dx, weight * dy, weight * dz
            new = (wx, wy, wz, weight * du, weight * dv, weight * dw, radial * wx, radial * wy, radial * wz)
            return tuple(s + n for s, n in zip(sums_here, new))

        zero = jnp.zeros((8, LANES), jnp.float32)
        got = lax.fori_loop(0, n_field, one_chunk, (zero,) * 9, unroll=4)
        for c in range(3):
            sums[c, at, :] = got[c]
            sums[3 + c, at, :] = got[3 + c] - 3.0 * got[6 + c]
        return carry

    lax.fori_loop(0, (total + 7) // 8, one_block, 0)
    folded = jnp.zeros((8, WIDE), jnp.float32)
    for c in range(6):
        ones = (row_iota((8, LANES)) == c).astype(jnp.float32)
        row = lax.dot_general(
            ones, sums[c], (((1,), (1,)), ((), ())), precision=EXACT, preferred_element_type=jnp.float32
        )
        row = jnp.where(row_iota((8, WIDE)) == c, row, 0.0)
        folded = folded + (pltpu.roll(row, SLOTS * c, 1) if c else row)
    lane = lane_iota((8, LANES))
    owned = own_rows((8, LANES))
    for k in range(n_line):
        moved = (pltpu.roll(folded, WIDE - starts[k], 1) if k else folded)[:, :LANES]
        kept = jnp.where(owned & (lane % SLOTS < lives[k]), moved, 0.0)
        packed = jnp.sum(kept, axis=0, keepdims=True)
        out[2 * k] = packed
        out[2 * k + 1] = packed


def correct_kernel(count, parts, pos, vel, acc, jerk, index, new_pos, new_vel, new_acc, new_jerk, slots):
    y, x, z = line_base()
    live = count[(y * lax.axis_size(X) + x) * lax.axis_size(Z) + z]
    force = parts[0]
    for k in range(1, parts.shape[0]):
        force = force + parts[k]
    shape = (8, LANES)
    lane = lane_iota(shape)
    spread = jnp.where(own_rows(shape), jnp.broadcast_to(force, shape), 0.0)
    spread = jnp.where((row_iota(shape) == 6) & own_rows(shape), 1.0, spread)
    table = (pos.shape[1], LANES)
    chosen = (row_iota(table) == tiled_slots(index, slots)) & (lane_iota(table) % SLOTS < live)
    placed = lax.dot_general(
        spread, chosen.astype(jnp.float32), (((1,), (1,)), ((), ())), precision=EXACT, preferred_element_type=jnp.float32
    )
    hit = jnp.broadcast_to(placed[6:7], (3, placed.shape[1])) > 0.5
    acc_one, jerk_one = placed[0:3], placed[3:6]
    pos_zero, vel_zero, acc_zero, jerk_zero = pos[...], vel[...], acc[...], jerk[...]
    twelfth = STEP_TIME * STEP_TIME / 12.0
    vel_one = vel_zero + (acc_zero + acc_one) * (STEP_TIME / 2.0) + (jerk_zero - jerk_one) * twelfth
    pos_one = pos_zero + (vel_zero + vel_one) * (STEP_TIME / 2.0) + (acc_zero - acc_one) * twelfth
    new_pos[...] = jnp.where(hit, pos_one, pos_zero)
    new_vel[...] = jnp.where(hit, vel_one, vel_zero)
    new_acc[...] = jnp.where(hit, acc_one, acc_zero)
    new_jerk[...] = jnp.where(hit, jerk_one, jerk_zero)


def f32(*shape):
    return jax.ShapeDtypeStruct(shape, jnp.float32)


VMEM = pl.BlockSpec(memory_space=pltpu.VMEM)
HBM = pl.BlockSpec(memory_space=pltpu.HBM)
SMEM = pl.BlockSpec(memory_space=pltpu.SMEM)


def shards(star_pos, star_vel, star_acc, star_jerk, masses, act_index, act_count):
    n_field = lax.axis_size(FIELD_AXES)
    n_line = lax.axis_size(ACT_AXIS)
    state = (star_pos, star_vel, star_acc, star_jerk)
    width = star_pos.shape[1]

    def line():
        y, x, z = line_base()
        return x * lax.axis_size(Z) + z, lax.axis_size(X) * lax.axis_size(Z)

    field, act = pl.pallas_call(
        prepare_kernel,
        out_shape=(pltpu.VMEM((n_field, 8, LANES), jnp.float32), pltpu.VMEM((1, LANES), jnp.float32)),
        in_specs=[HBM] * 6,
        out_specs=(VMEM, VMEM),
        scratch_shapes=[pltpu.VMEM((3, width), jnp.float32)] * 4
        + [
            pltpu.VMEM((1, width), jnp.float32),
            pltpu.VMEM((1, SLOTS), jnp.int32),
            pltpu.VMEM((8, width), jnp.float32),
            pltpu.VMEM((8, LANES), jnp.int32),
            pltpu.SemaphoreType.DMA((6,)),
        ],
        compiler_params=pltpu.CompilerParams(vmem_limit_bytes=LIMIT),
        name="prepare",
    )(*[pltpu.with_memory_space_constraint(a, pltpu.HBM) for a in (*state, masses[None, :], act_index)])
    field = lax.all_to_all(field, FIELD_AXES, 0, 0, tiled=True)
    act = lax.all_gather(act, ACT_AXIS)
    parts = pl.pallas_call(
        lambda *refs: forces_kernel(line, *refs),
        out_shape=f32(2 * n_line, 1, LANES),
        in_specs=[SMEM, VMEM, VMEM],
        out_specs=VMEM,
        scratch_shapes=[
            pltpu.VMEM((16, LANES), jnp.float32),
            pltpu.VMEM((6, WIDE, LANES), jnp.float32),
            pltpu.VMEM((6, WIDE, LANES), jnp.float32),
        ],
        compiler_params=pltpu.CompilerParams(vmem_limit_bytes=LIMIT),
        name="forces",
    )(act_count, field, act)
    parts = lax.all_to_all(parts, (ACT_AXIS, REP), 0, 0, tiled=True)
    return pl.pallas_call(
        correct_kernel,
        out_shape=tuple(f32(3, width) for _ in range(4)),
        in_specs=[SMEM] + [VMEM] * 6,
        out_specs=(VMEM,) * 4,
        scratch_shapes=[pltpu.VMEM((8, LANES), jnp.int32)],
        compiler_params=pltpu.CompilerParams(vmem_limit_bytes=LIMIT),
        name="correct",
    )(act_count, parts, *state, act_index)


def solution(mesh):
    finer = Mesh(mesh.devices.reshape(8, 4, 12, mesh.shape["rep"]), (Y, X, Z, REP))
    placed = (P(None, BLK), P(None, BLK), P(None, BLK), P(None, BLK), P(BLK), P(BLK, None), P())
    return jax.shard_map(
        shards,
        mesh=finer,
        in_specs=placed,
        out_specs=(P(None, BLK), P(None, BLK), P(None, BLK), P(None, BLK)),
        check_vma=False,
    )
```

```python
import jax
import jax.numpy as jnp
from jax import lax
from jax.experimental import pallas as pl
from jax.experimental.pallas import tpu as pltpu
from jax.sharding import Mesh
from jax.sharding import PartitionSpec as P

Y, X, Z, REP = "blk_0", "blk_1", "blk_2", "rep"
BLK = (Y, X, Z)
FIELD_AXES = (Y, Z)
ACT_AXIS = X

STEP_TIME = 0.0625
SOFTEN_SQ = 0.0001
HALF_SQ = STEP_TIME * STEP_TIME / 2.0
LANES = 128
SLOTS = 16
WIDE = 128
ROWS = 7
LIMIT = 8 * 1024 * 1024
EXACT = lax.Precision.HIGHEST


def lane_iota(shape):
    return lax.broadcasted_iota(jnp.int32, shape, len(shape) - 1)


def row_iota(shape):
    return lax.broadcasted_iota(jnp.int32, shape, len(shape) - 2)


def tiled_slots(index_ref, scratch):
    scratch[...] = jnp.zeros(scratch.shape, jnp.int32)
    scratch[0:1, 0:SLOTS] = index_ref[...]
    row = scratch[0:1, :]
    for shift in (16, 32, 64):
        row = row + pltpu.roll(row, shift, 1)
    return row


def own_rows(shape):
    return row_iota(shape) == lane_iota(shape) // SLOTS


def prepare_kernel(*refs):
    given, (field_out, act_out), (pos, vel, acc, jerk, mass, index, state, slots, done) = refs[:6], refs[6:8], refs[8:]
    copies = [
        pltpu.make_async_copy(far, near, done.at[k])
        for k, (far, near) in enumerate(zip(given, (pos, vel, acc, jerk, mass, index)))
    ]
    for copy in copies:
        copy.start()
    for copy in copies:
        copy.wait()
    cubed = STEP_TIME * HALF_SQ / 3.0
    state[0:3, :] = pos[...] + STEP_TIME * vel[...] + HALF_SQ * acc[...] + cubed * jerk[...]
    state[3:6, :] = vel[...] + STEP_TIME * acc[...] + HALF_SQ * jerk[...]
    state[6:7, :] = mass[...]
    state[7:8, :] = jnp.zeros((1, state.shape[1]), jnp.float32)
    whole = state[...]
    half = jnp.where(lax.axis_index(REP) == 0, whole[:ROWS, :LANES], whole[:ROWS, LANES:])
    for k in range(field_out.shape[0]):
        field_out[k] = half
    shape = (whole.shape[1], LANES)
    chosen = (row_iota(shape) == tiled_slots(index, slots)).astype(jnp.float32)
    picked = jnp.dot(whole, chosen, precision=EXACT, preferred_element_type=jnp.float32)
    packed = jnp.sum(jnp.where(own_rows(picked.shape), picked, 0.0), axis=0, keepdims=True)
    act_out[...] = packed


def line_base():
    y, x, z = lax.axis_index(Y), lax.axis_index(X), lax.axis_index(Z)
    return y, x, z


def forces_kernel(line, count, field, act, out, rows, active, sums):
    n_line = act.shape[0]
    n_field = field.shape[0]
    first, stride = line()
    rows[...] = jnp.zeros(rows.shape, jnp.float32)
    for k in range(n_line):
        rows[k : k + 1, :] = act[k]
    columns = rows[...].T
    starts = []
    lives = []
    total = 0
    for k in range(n_line):
        live = count[first + k * stride]
        starts.append(total)
        lives.append(live)
        total = total + live
    for k in range(n_line):
        spread = jnp.broadcast_to(columns[0:96, k : k + 1], (96, LANES))
        for c in range(6):
            active[c, pl.ds(starts[k], SLOTS), :] = spread[c * SLOTS : (c + 1) * SLOTS]

    def one_block(b, carry):
        at = pl.ds(pl.multiple_of(b * 8, 8), 8)
        mine = [active[c, at, :] for c in range(6)]

        def one_chunk(f, sums_here):
            def row(c):
                return jnp.broadcast_to(field[f, c : c + 1, :], (8, LANES))

            dx, dy, dz, du, dv, dw = [row(c) - mine[c] for c in range(6)]
            radius_sq = dx * dx + dy * dy + dz * dz + SOFTEN_SQ
            root = lax.rsqrt(radius_sq)
            inverse = root * root
            weight = row(6) * root * inverse
            radial = (dx * du + dy * dv + dz * dw) * inverse
            wx, wy, wz = weight * dx, weight * dy, weight * dz
            new = (wx, wy, wz, weight * du, weight * dv, weight * dw, radial * wx, radial * wy, radial * wz)
            return tuple(s + n for s, n in zip(sums_here, new))

        zero = jnp.zeros((8, LANES), jnp.float32)
        got = lax.fori_loop(0, n_field, one_chunk, (zero,) * 9, unroll=4)
        for c in range(3):
            sums[c, at, :] = got[c]
            sums[3 + c, at, :] = got[3 + c] - 3.0 * got[6 + c]
        return carry

    lax.fori_loop(0, (total + 7) // 8, one_block, 0)
    folded = jnp.zeros((8, WIDE), jnp.float32)
    for c in range(6):
        ones = (row_iota((8, LANES)) == c).astype(jnp.float32)
        row = lax.dot_general(
            ones, sums[c], (((1,), (1,)), ((), ())), precision=EXACT, preferred_element_type=jnp.float32
        )
        row = jnp.where(row_iota((8, WIDE)) == c, row, 0.0)
        folded = folded + (pltpu.roll(row, SLOTS * c, 1) if c else row)
    lane = lane_iota((8, LANES))
    owned = own_rows((8, LANES))
    for k in range(n_line):
        moved = (pltpu.roll(folded, WIDE - starts[k], 1) if k else folded)[:, :LANES]
        kept = jnp.where(owned & (lane % SLOTS < lives[k]), moved, 0.0)
        packed = jnp.sum(kept, axis=0, keepdims=True)
        out[2 * k] = packed
        out[2 * k + 1] = packed


def correct_kernel(count, parts, pos, vel, acc, jerk, index, new_pos, new_vel, new_acc, new_jerk, slots):
    y, x, z = line_base()
    live = count[(y * lax.axis_size(X) + x) * lax.axis_size(Z) + z]
    force = parts[0]
    for k in range(1, parts.shape[0]):
        force = force + parts[k]
    shape = (8, LANES)
    lane = lane_iota(shape)
    spread = jnp.where(own_rows(shape), jnp.broadcast_to(force, shape), 0.0)
    spread = jnp.where((row_iota(shape) == 6) & own_rows(shape), 1.0, spread)
    table = (pos.shape[1], LANES)
    chosen = (row_iota(table) == tiled_slots(index, slots)) & (lane_iota(table) % SLOTS < live)
    placed = lax.dot_general(
        spread, chosen.astype(jnp.float32), (((1,), (1,)), ((), ())), precision=EXACT, preferred_element_type=jnp.float32
    )
    hit = jnp.broadcast_to(placed[6:7], (3, placed.shape[1])) > 0.5
    acc_one, jerk_one = placed[0:3], placed[3:6]
    pos_zero, vel_zero, acc_zero, jerk_zero = pos[...], vel[...], acc[...], jerk[...]
    twelfth = STEP_TIME * STEP_TIME / 12.0
    vel_one = vel_zero + (acc_zero + acc_one) * (STEP_TIME / 2.0) + (jerk_zero - jerk_one) * twelfth
    pos_one = pos_zero + (vel_zero + vel_one) * (STEP_TIME / 2.0) + (acc_zero - acc_one) * twelfth
    new_pos[...] = jnp.where(hit, pos_one, pos_zero)
    new_vel[...] = jnp.where(hit, vel_one, vel_zero)
    new_acc[...] = jnp.where(hit, acc_one, acc_zero)
    new_jerk[...] = jnp.where(hit, jerk_one, jerk_zero)


def f32(*shape):
    return jax.ShapeDtypeStruct(shape, jnp.float32)


VMEM = pl.BlockSpec(memory_space=pltpu.VMEM)
HBM = pl.BlockSpec(memory_space=pltpu.HBM)
SMEM = pl.BlockSpec(memory_space=pltpu.SMEM)


def shards(star_pos, star_vel, star_acc, star_jerk, masses, act_index, act_count):
    n_field = lax.axis_size(FIELD_AXES)
    n_line = lax.axis_size(ACT_AXIS)
    state = (star_pos, star_vel, star_acc, star_jerk)
    width = star_pos.shape[1]

    def line():
        y, x, z = line_base()
        return y * lax.axis_size(X) * lax.axis_size(Z) + z, lax.axis_size(Z)

    field, act = pl.pallas_call(
        prepare_kernel,
        out_shape=(pltpu.VMEM((n_field, ROWS, LANES), jnp.float32), pltpu.VMEM((1, LANES), jnp.float32)),
        in_specs=[HBM] * 6,
        out_specs=(VMEM, VMEM),
        scratch_shapes=[pltpu.VMEM((3, width), jnp.float32)] * 4
        + [
            pltpu.VMEM((1, width), jnp.float32),
            pltpu.VMEM((1, SLOTS), jnp.int32),
            pltpu.VMEM((8, width), jnp.float32),
            pltpu.VMEM((8, LANES), jnp.int32),
            pltpu.SemaphoreType.DMA((6,)),
        ],
        compiler_params=pltpu.CompilerParams(vmem_limit_bytes=LIMIT),
        name="prepare",
    )(*[pltpu.with_memory_space_constraint(a, pltpu.HBM) for a in (*state, masses[None, :], act_index)])
    field = lax.all_to_all(field, FIELD_AXES, 0, 0, tiled=True)
    act = lax.all_gather(act, ACT_AXIS)
    parts = pl.pallas_call(
        lambda *refs: forces_kernel(line, *refs),
        out_shape=f32(2 * n_line, 1, LANES),
        in_specs=[SMEM, VMEM, VMEM],
        out_specs=VMEM,
        scratch_shapes=[
            pltpu.VMEM((16, LANES), jnp.float32),
            pltpu.VMEM((6, WIDE, LANES), jnp.float32),
            pltpu.VMEM((6, WIDE, LANES), jnp.float32),
        ],
        compiler_params=pltpu.CompilerParams(vmem_limit_bytes=LIMIT),
        name="forces",
    )(act_count, field, act)
    parts = lax.all_to_all(parts, (ACT_AXIS, REP), 0, 0, tiled=True)
    return pl.pallas_call(
        correct_kernel,
        out_shape=tuple(f32(3, width) for _ in range(4)),
        in_specs=[SMEM] + [VMEM] * 6,
        out_specs=(VMEM,) * 4,
        scratch_shapes=[pltpu.VMEM((8, LANES), jnp.int32)],
        compiler_params=pltpu.CompilerParams(vmem_limit_bytes=LIMIT),
        name="correct",
    )(act_count, parts, *state, act_index)


def solution(mesh):
    finer = Mesh(mesh.devices.reshape(8, 4, 12, mesh.shape["rep"]), (Y, X, Z, REP))
    placed = (P(None, BLK), P(None, BLK), P(None, BLK), P(None, BLK), P(BLK), P(BLK, None), P())
    return jax.shard_map(
        shards,
        mesh=finer,
        in_specs=placed,
        out_specs=(P(None, BLK), P(None, BLK), P(None, BLK), P(None, BLK)),
        check_vma=False,
    )
```

```python
import jax
import jax.numpy as jnp
from jax import lax
from jax.experimental import pallas as pl
from jax.experimental.pallas import tpu as pltpu
from jax.sharding import Mesh
from jax.sharding import PartitionSpec as P

Y, X, Z, REP = "blk_0", "blk_1", "blk_2", "rep"
BLK = (Y, X, Z)
FIELD_AXES = (X, Z)
ACT_AXIS = Y

STEP_TIME = 0.0625
SOFTEN_SQ = 0.0001
HALF_SQ = STEP_TIME * STEP_TIME / 2.0
LANES = 128
SLOTS = 16
WIDE = 128
LIMIT = 8 * 1024 * 1024
UNROLL = 12


def lane_iota(shape):
    return lax.broadcasted_iota(jnp.int32, shape, len(shape) - 1)


def row_iota(shape):
    return lax.broadcasted_iota(jnp.int32, shape, len(shape) - 2)


def tiled_slots(index_ref, scratch):
    scratch[...] = jnp.zeros(scratch.shape, jnp.int32)
    scratch[0:1, 0:SLOTS] = index_ref[...]
    row = scratch[0:1, :]
    for shift in (16, 32, 64):
        row = row + pltpu.roll(row, shift, 1)
    return row


def own_rows(shape):
    return row_iota(shape) == lane_iota(shape) // SLOTS


def prepare_kernel(*refs):
    given, (field_out, act_out), (pos, vel, acc, jerk, mass, index, state, slots, done) = refs[:6], refs[6:8], refs[8:]
    copies = [
        pltpu.make_async_copy(far, near, done.at[k])
        for k, (far, near) in enumerate(zip(given, (pos, vel, acc, jerk, mass, index)))
    ]
    for copy in copies:
        copy.start()
    for copy in copies:
        copy.wait()
    cubed = STEP_TIME * HALF_SQ / 3.0
    state[0:3, :] = pos[...] + STEP_TIME * vel[...] + HALF_SQ * acc[...] + cubed * jerk[...]
    state[3:6, :] = vel[...] + STEP_TIME * acc[...] + HALF_SQ * jerk[...]
    state[6:7, :] = mass[...]
    state[7:8, :] = jnp.zeros((1, state.shape[1]), jnp.float32)
    whole = state[...]
    half = jnp.where(lax.axis_index(REP) == 0, whole[:, :LANES], whole[:, LANES:])
    for k in range(field_out.shape[0]):
        field_out[k] = half
    shape = (whole.shape[1], LANES)
    chosen = (row_iota(shape) == tiled_slots(index, slots)).astype(jnp.bfloat16)
    picked = jnp.zeros((8, LANES), jnp.float32)
    for part in exact_parts(whole):
        picked = picked + jnp.dot(part, chosen, preferred_element_type=jnp.float32)
    packed = jnp.sum(jnp.where(own_rows(picked.shape), picked, 0.0), axis=0, keepdims=True)
    act_out[...] = packed


def line_base():
    y, x, z = lax.axis_index(Y), lax.axis_index(X), lax.axis_index(Z)
    return y, x, z


def exact_parts(value):
    high = value.astype(jnp.bfloat16)
    rest = value - high.astype(jnp.float32)
    middle = rest.astype(jnp.bfloat16)
    low = (rest - middle.astype(jnp.float32)).astype(jnp.bfloat16)
    return high, middle, low


def spread_kernel(line, count, index, act, active, meta, table, rows, slots):
    y, x, z = line_base()
    live = count[(y * lax.axis_size(X) + x) * lax.axis_size(Z) + z]
    stars = jnp.broadcast_to(tiled_slots(index, slots), (8, LANES)).astype(jnp.float32).T[:, 0:1]
    shape = (LANES, table.shape[1])
    here = jnp.broadcast_to(stars, shape) == lane_iota(shape).astype(jnp.float32)
    table[...] = (here & (row_iota(shape) % SLOTS < live)).astype(jnp.bfloat16)
    n_line = act.shape[0]
    first, stride = line()
    rows[...] = jnp.zeros(rows.shape, jnp.float32)
    for k in range(n_line):
        rows[k : k + 1, :] = act[k]
    columns = rows[...].T
    lane, row = lane_iota((8, LANES)), row_iota((8, LANES))
    known = jnp.zeros((8, LANES), jnp.int32)
    start = 0
    for k in range(n_line):
        live = count[first + k * stride]
        known = jnp.where((row == 0) & (lane == k), start, known)
        known = jnp.where((row == 1) & (lane == k), live, known)
        spread = jnp.broadcast_to(columns[0:96, k : k + 1], (96, LANES))
        for c in range(6):
            active[c, pl.ds(start, SLOTS), :] = spread[c * SLOTS : (c + 1) * SLOTS]
        start = start + live
    meta[...] = jnp.where(row == 2, start, known)


def forces_kernel(meta, field, active, out, sums, known, done):
    n_line = out.shape[0] // 2
    n_field = field.shape[0]
    copy = pltpu.make_async_copy(meta, known, done)
    copy.start()
    total = jnp.max(meta[2:3, :])

    def one_block(b, carry):
        at = pl.ds(pl.multiple_of(b * 8, 8), 8)
        mine = [active[c, at, :] for c in range(6)]

        def one_chunk(f, sums_here):
            def row(c):
                return jnp.broadcast_to(field[f, c : c + 1, :], (8, LANES))

            dx, dy, dz, du, dv, dw = [row(c) - mine[c] for c in range(6)]
            radius_sq = (dx * dx + dy * dy) + (dz * dz + SOFTEN_SQ)
            root = lax.rsqrt(radius_sq)
            inverse = root * root
            weight = (row(6) * root) * inverse
            radial = (dx * du + dy * dv + dz * dw) * inverse
            wx, wy, wz = weight * dx, weight * dy, weight * dz
            new = (wx, wy, wz, weight * du, weight * dv, weight * dw, radial * wx, radial * wy, radial * wz)
            return tuple(s + n for s, n in zip(sums_here, new))

        zero = jnp.zeros((8, LANES), jnp.float32)
        got = lax.fori_loop(0, n_field, one_chunk, (zero,) * 9, unroll=UNROLL)
        for c in range(3):
            sums[c, at, :] = got[c]
            sums[3 + c, at, :] = got[3 + c] - 3.0 * got[6 + c]
        return carry

    lax.fori_loop(0, (total + 7) // 8, one_block, 0)
    folded = jnp.zeros((8, WIDE), jnp.float32)
    for c in range(6):
        ones = (row_iota((8, LANES)) == c).astype(jnp.bfloat16)
        row = jnp.zeros((8, WIDE), jnp.float32)
        for part in exact_parts(sums[c]):
            row = row + lax.dot_general(ones, part, (((1,), (1,)), ((), ())), preferred_element_type=jnp.float32)
        row = jnp.where(row_iota((8, WIDE)) == c, row, 0.0)
        folded = folded + (pltpu.roll(row, SLOTS * c, 1) if c else row)
    lane = lane_iota((8, LANES))
    owned = own_rows((8, LANES))
    copy.wait()
    for k in range(n_line):
        moved = pltpu.roll(folded, WIDE - known[0, k], 1) if k else folded
        kept = jnp.where(owned & (lane % SLOTS < known[1, k]), moved, 0.0)
        packed = jnp.sum(kept, axis=0, keepdims=True)
        out[2 * k] = packed
        out[2 * k + 1] = packed


def correct_kernel(table, parts, pos, vel, acc, jerk, new_pos, new_vel, new_acc, new_jerk):
    force = parts[0]
    for k in range(1, parts.shape[0]):
        force = force + parts[k]
    shape = (8, LANES)
    spread = jnp.where(own_rows(shape), jnp.broadcast_to(force, shape), 0.0)
    spread = jnp.where((row_iota(shape) == 6) & own_rows(shape), 1.0, spread)
    placed = jnp.zeros((8, table.shape[1]), jnp.float32)
    for part in exact_parts(spread):
        placed = placed + jnp.dot(part, table[...], preferred_element_type=jnp.float32)
    hit = jnp.broadcast_to(placed[6:7], (3, placed.shape[1])) > 0.5
    acc_one, jerk_one = placed[0:3], placed[3:6]
    pos_zero, vel_zero, acc_zero, jerk_zero = pos[...], vel[...], acc[...], jerk[...]
    twelfth = STEP_TIME * STEP_TIME / 12.0
    vel_one = vel_zero + (acc_zero + acc_one) * (STEP_TIME / 2.0) + (jerk_zero - jerk_one) * twelfth
    pos_one = pos_zero + (vel_zero + vel_one) * (STEP_TIME / 2.0) + (acc_zero - acc_one) * twelfth
    new_pos[...] = jnp.where(hit, pos_one, pos_zero)
    new_vel[...] = jnp.where(hit, vel_one, vel_zero)
    new_acc[...] = jnp.where(hit, acc_one, acc_zero)
    new_jerk[...] = jnp.where(hit, jerk_one, jerk_zero)


def f32(*shape):
    return jax.ShapeDtypeStruct(shape, jnp.float32)


VMEM = pl.BlockSpec(memory_space=pltpu.VMEM)
HBM = pl.BlockSpec(memory_space=pltpu.HBM)
SMEM = pl.BlockSpec(memory_space=pltpu.SMEM)


def shards(star_pos, star_vel, star_acc, star_jerk, masses, act_index, act_count):
    n_field = lax.axis_size(FIELD_AXES)
    n_line = lax.axis_size(ACT_AXIS)
    state = (star_pos, star_vel, star_acc, star_jerk)
    width = star_pos.shape[1]

    def line():
        y, x, z = line_base()
        return x * lax.axis_size(Z) + z, lax.axis_size(X) * lax.axis_size(Z)

    field, act = pl.pallas_call(
        prepare_kernel,
        out_shape=(pltpu.VMEM((n_field, 8, LANES), jnp.float32), pltpu.VMEM((1, LANES), jnp.float32)),
        in_specs=[HBM] * 6,
        out_specs=(VMEM, VMEM),
        scratch_shapes=[pltpu.VMEM((3, width), jnp.float32)] * 4
        + [
            pltpu.VMEM((1, width), jnp.float32),
            pltpu.VMEM((1, SLOTS), jnp.int32),
            pltpu.VMEM((8, width), jnp.float32),
            pltpu.VMEM((8, LANES), jnp.int32),
            pltpu.SemaphoreType.DMA((6,)),
        ],
        compiler_params=pltpu.CompilerParams(vmem_limit_bytes=LIMIT),
        name="prepare",
    )(*[pltpu.with_memory_space_constraint(a, pltpu.HBM) for a in (*state, masses[None, :], act_index)])
    field = lax.all_to_all(field, FIELD_AXES, 0, 0, tiled=True)
    act = lax.all_gather(act, ACT_AXIS)
    call = dict(compiler_params=pltpu.CompilerParams(vmem_limit_bytes=LIMIT))
    active, meta, table = pl.pallas_call(
        lambda *refs: spread_kernel(line, *refs),
        out_shape=(pltpu.VMEM((6, WIDE + SLOTS, LANES), jnp.float32), pltpu.VMEM((8, LANES), jnp.int32), pltpu.VMEM((LANES, width), jnp.bfloat16)),
        in_specs=[SMEM, VMEM, VMEM],
        out_specs=(VMEM,) * 3,
        scratch_shapes=[pltpu.VMEM((8, LANES), jnp.float32), pltpu.VMEM((8, LANES), jnp.int32)],
        name="spread",
        **call,
    )(act_count, act_index, act)
    parts = pl.pallas_call(
        forces_kernel,
        out_shape=pltpu.VMEM((2 * n_line, 1, LANES), jnp.float32),
        in_specs=[VMEM] * 3,
        out_specs=VMEM,
        scratch_shapes=[
            pltpu.VMEM((6, WIDE, LANES), jnp.float32),
            pltpu.SMEM((8, LANES), jnp.int32),
            pltpu.SemaphoreType.DMA(()),
        ],
        name="forces",
        **call,
    )(meta, field, active)
    parts = lax.all_to_all(parts, (ACT_AXIS, REP), 0, 0, tiled=True)
    return pl.pallas_call(
        correct_kernel,
        out_shape=tuple(f32(3, width) for _ in range(4)),
        in_specs=[VMEM] * 6,
        out_specs=(VMEM,) * 4,
        name="correct",
        **call,
    )(table, parts, *state)


def solution(mesh):
    finer = Mesh(mesh.devices.reshape(8, 4, 12, mesh.shape["rep"]), (Y, X, Z, REP))
    placed = (P(None, BLK), P(None, BLK), P(None, BLK), P(None, BLK), P(BLK), P(BLK, None), P())
    return jax.shard_map(
        shards,
        mesh=finer,
        in_specs=placed,
        out_specs=(P(None, BLK), P(None, BLK), P(None, BLK), P(None, BLK)),
        check_vma=False,
    )
```

```python
import jax
import jax.numpy as jnp
from jax import lax
from jax.experimental import pallas as pl
from jax.experimental.pallas import tpu as pltpu
from jax.sharding import Mesh
from jax.sharding import PartitionSpec as P

Y, X, Z, REP = "blk_0", "blk_1", "blk_2", "rep"
BLK = (Y, X, Z)
FIELD_AXES = (X, Z)
ACT_AXIS = Y

STEP_TIME = 0.0625
SOFTEN_SQ = 0.0001
HALF_SQ = STEP_TIME * STEP_TIME / 2.0
LANES = 128
SLOTS = 16
WIDE = 128
LIMIT = 8 * 1024 * 1024
UNROLL = 12


def lane_iota(shape):
    return lax.broadcasted_iota(jnp.int32, shape, len(shape) - 1)


def row_iota(shape):
    return lax.broadcasted_iota(jnp.int32, shape, len(shape) - 2)


def tiled_slots(index_ref, scratch):
    scratch[...] = jnp.zeros(scratch.shape, jnp.int32)
    scratch[0:1, 0:SLOTS] = index_ref[...]
    row = scratch[0:1, :]
    for shift in (16, 32, 64):
        row = row + pltpu.roll(row, shift, 1)
    return row


def own_rows(shape):
    return row_iota(shape) == lane_iota(shape) // SLOTS


def prepare_kernel(line, *refs):
    given, (field_out, act_out, meta, table) = refs[:7], refs[7:11]
    pos, vel, acc, jerk, mass, index, count, state, slots, done = refs[11:]
    copies = [
        pltpu.make_async_copy(far, near, done.at[k])
        for k, (far, near) in enumerate(zip(given, (pos, vel, acc, jerk, mass, index, count)))
    ]
    for copy in copies:
        copy.start()
    for copy in copies:
        copy.wait()
    cubed = STEP_TIME * HALF_SQ / 3.0
    state[0:3, :] = pos[...] + STEP_TIME * vel[...] + HALF_SQ * acc[...] + cubed * jerk[...]
    state[3:6, :] = vel[...] + STEP_TIME * acc[...] + HALF_SQ * jerk[...]
    state[6:7, :] = mass[...]
    state[7:8, :] = jnp.zeros((1, state.shape[1]), jnp.float32)
    whole = state[...]
    half = jnp.where(lax.axis_index(REP) == 0, whole[:, :LANES], whole[:, LANES:])
    for k in range(field_out.shape[0]):
        field_out[k] = half
    shape = (whole.shape[1], LANES)
    tiled = tiled_slots(index, slots)
    chosen = (row_iota(shape) == tiled).astype(jnp.bfloat16)
    picked = jnp.zeros((8, LANES), jnp.float32)
    for part in exact_parts(whole):
        picked = picked + jnp.dot(part, chosen, preferred_element_type=jnp.float32)
    packed = jnp.sum(jnp.where(own_rows(picked.shape), picked, 0.0), axis=0, keepdims=True)
    act_out[...] = packed
    first, stride = line()
    lane, row = lane_iota((8, LANES)), row_iota((8, LANES))
    known = jnp.zeros((8, LANES), jnp.int32)
    start = 0
    for k in range(lax.axis_size(ACT_AXIS)):
        live = count[first + k * stride]
        known = jnp.where((row == 0) & (lane == k), start, known)
        known = jnp.where((row == 1) & (lane == k), live, known)
        start = start + live
    meta[...] = jnp.where(row == 2, start, known)
    y, x, z = line_base()
    live = count[(y * lax.axis_size(X) + x) * lax.axis_size(Z) + z]
    stars = jnp.broadcast_to(tiled, (8, LANES)).astype(jnp.float32).T[:, 0:1]
    shape = (LANES, table.shape[1])
    here = jnp.broadcast_to(stars, shape) == lane_iota(shape).astype(jnp.float32)
    table[...] = (here & (row_iota(shape) % SLOTS < live)).astype(jnp.bfloat16)


def line_base():
    y, x, z = lax.axis_index(Y), lax.axis_index(X), lax.axis_index(Z)
    return y, x, z


def exact_parts(value):
    high = value.astype(jnp.bfloat16)
    rest = value - high.astype(jnp.float32)
    middle = rest.astype(jnp.bfloat16)
    low = (rest - middle.astype(jnp.float32)).astype(jnp.bfloat16)
    return high, middle, low


def spread_kernel(meta, act, active, rows):
    n_line = act.shape[0]
    rows[...] = jnp.zeros(rows.shape, jnp.float32)
    for k in range(n_line):
        rows[k : k + 1, :] = act[k]
    columns = rows[...].T
    lane = lane_iota((1, LANES))
    for k in range(n_line):
        start = jnp.max(jnp.where(lane == k, meta[0:1, :], 0)) if k else 0
        spread = jnp.broadcast_to(columns[0:96, k : k + 1], (96, LANES))
        for c in range(6):
            active[c, pl.ds(start, SLOTS), :] = spread[c * SLOTS : (c + 1) * SLOTS]


def forces_kernel(order, meta, field, active, out, sums, known, done):
    n_line = out.shape[0] // 2
    n_field = field.shape[0]
    copy = pltpu.make_async_copy(meta, known, done)
    copy.start()
    total = jnp.max(meta[2:3, :])

    def one_block(b, carry):
        at = pl.ds(pl.multiple_of(b * 8, 8), 8)
        mine = [active[c, at, :] for c in range(6)]

        def one_chunk(f, sums_here):
            def row(c):
                return jnp.broadcast_to(field[f, c : c + 1, :], (8, LANES))

            dx, dy, dz, du, dv, dw = [row(c) - mine[c] for c in range(6)]
            radius_sq = (dx * dx + dy * dy) + (dz * dz + SOFTEN_SQ)
            root = lax.rsqrt(radius_sq)
            inverse = root * root
            weight = (row(6) * root) * inverse
            radial = (dx * du + dy * dv + dz * dw) * inverse
            wx, wy, wz = weight * dx, weight * dy, weight * dz
            new = (wx, wy, wz, weight * du, weight * dv, weight * dw, radial * wx, radial * wy, radial * wz)
            return tuple(s + n for s, n in zip(sums_here, new))

        zero = jnp.zeros((8, LANES), jnp.float32)
        got = lax.fori_loop(0, n_field, one_chunk, (zero,) * 9, unroll=UNROLL)
        for c in range(3):
            sums[c, at, :] = got[c]
            sums[3 + c, at, :] = got[3 + c] - 3.0 * got[6 + c]
        return carry

    lax.fori_loop(0, (total + 7) // 8, one_block, 0)
    folded = jnp.zeros((8, WIDE), jnp.float32)
    for c in range(6):
        ones = (row_iota((8, LANES)) == c).astype(jnp.bfloat16)
        row = jnp.zeros((8, WIDE), jnp.float32)
        for part in exact_parts(sums[c]):
            row = row + lax.dot_general(ones, part, (((1,), (1,)), ((), ())), preferred_element_type=jnp.float32)
        row = jnp.where(row_iota((8, WIDE)) == c, row, 0.0)
        folded = folded + (pltpu.roll(row, SLOTS * c, 1) if c else row)
    lane = lane_iota((8, LANES))
    owned = own_rows((8, LANES))
    copy.wait()
    for k in range(n_line):
        moved = pltpu.roll(folded, WIDE - known[0, k], 1) if k else folded
        kept = jnp.where(owned & (lane % SLOTS < known[1, k]), moved, 0.0)
        packed = jnp.sum(kept, axis=0, keepdims=True)
        for j, member in enumerate(order):
            if member // 2 == k:
                out[j] = packed


def correct_kernel(table, parts, pos, vel, acc, jerk, new_pos, new_vel, new_acc, new_jerk):
    force = parts[0]
    for k in range(1, parts.shape[0]):
        force = force + parts[k]
    shape = (8, LANES)
    spread = jnp.where(own_rows(shape), jnp.broadcast_to(force, shape), 0.0)
    spread = jnp.where((row_iota(shape) == 6) & own_rows(shape), 1.0, spread)
    placed = jnp.zeros((8, table.shape[1]), jnp.float32)
    for part in exact_parts(spread):
        placed = placed + jnp.dot(part, table[...], preferred_element_type=jnp.float32)
    hit = jnp.broadcast_to(placed[6:7], (3, placed.shape[1])) > 0.5
    acc_one, jerk_one = placed[0:3], placed[3:6]
    pos_zero, vel_zero, acc_zero, jerk_zero = pos[...], vel[...], acc[...], jerk[...]
    twelfth = STEP_TIME * STEP_TIME / 12.0
    vel_one = vel_zero + (acc_zero + acc_one) * (STEP_TIME / 2.0) + (jerk_zero - jerk_one) * twelfth
    pos_one = pos_zero + (vel_zero + vel_one) * (STEP_TIME / 2.0) + (acc_zero - acc_one) * twelfth
    new_pos[...] = jnp.where(hit, pos_one, pos_zero)
    new_vel[...] = jnp.where(hit, vel_one, vel_zero)
    new_acc[...] = jnp.where(hit, acc_one, acc_zero)
    new_jerk[...] = jnp.where(hit, jerk_one, jerk_zero)


def f32(*shape):
    return jax.ShapeDtypeStruct(shape, jnp.float32)


VMEM = pl.BlockSpec(memory_space=pltpu.VMEM)
HBM = pl.BlockSpec(memory_space=pltpu.HBM)


def shards(star_pos, star_vel, star_acc, star_jerk, masses, act_index, act_count):
    n_field = lax.axis_size(FIELD_AXES)
    n_line = lax.axis_size(ACT_AXIS)
    state = (star_pos, star_vel, star_acc, star_jerk)
    width = star_pos.shape[1]

    def line():
        y, x, z = line_base()
        return x * lax.axis_size(Z) + z, lax.axis_size(X) * lax.axis_size(Z)

    given = (*state, masses[None, :], act_index, act_count)
    call = dict(compiler_params=pltpu.CompilerParams(vmem_limit_bytes=LIMIT))
    field, act, meta, table = pl.pallas_call(
        lambda *refs: prepare_kernel(line, *refs),
        out_shape=(
            pltpu.VMEM((n_field, 8, LANES), jnp.float32),
            pltpu.VMEM((1, LANES), jnp.float32),
            pltpu.VMEM((8, LANES), jnp.int32),
            pltpu.VMEM((LANES, width), jnp.bfloat16),
        ),
        in_specs=[HBM] * 7,
        out_specs=(VMEM,) * 4,
        scratch_shapes=[pltpu.VMEM((3, width), jnp.float32)] * 4
        + [
            pltpu.VMEM((1, width), jnp.float32),
            pltpu.VMEM((1, SLOTS), jnp.int32),
            pltpu.SMEM(act_count.shape, jnp.int32),
            pltpu.VMEM((8, width), jnp.float32),
            pltpu.VMEM((8, LANES), jnp.int32),
            pltpu.SemaphoreType.DMA((7,)),
        ],
        name="prepare",
        **call,
    )(*[pltpu.with_memory_space_constraint(a, pltpu.HBM) for a in given])
    field = lax.all_to_all(field, FIELD_AXES, 0, 0, tiled=True)
    act = lax.all_gather(act, ACT_AXIS)
    active = pl.pallas_call(
        spread_kernel,
        out_shape=pltpu.VMEM((6, WIDE + SLOTS, LANES), jnp.float32),
        in_specs=[VMEM] * 2,
        out_specs=VMEM,
        scratch_shapes=[pltpu.VMEM((8, LANES), jnp.float32)],
        name="spread",
        **call,
    )(meta, act)
    order = [2 * ((j // 2 + n_line // 2) % n_line) + 1 - j % 2 for j in range(2 * n_line)]
    parts = pl.pallas_call(
        lambda *refs: forces_kernel(order, *refs),
        out_shape=pltpu.VMEM((2 * n_line, 1, LANES), jnp.float32),
        in_specs=[VMEM] * 3,
        out_specs=VMEM,
        scratch_shapes=[
            pltpu.VMEM((6, WIDE, LANES), jnp.float32),
            pltpu.SMEM((8, LANES), jnp.int32),
            pltpu.SemaphoreType.DMA(()),
        ],
        name="forces",
        **call,
    )(meta, field, active)
    parts = lax.all_to_all(parts, (ACT_AXIS, REP), 0, 0, axis_index_groups=[order], tiled=True)
    return pl.pallas_call(
        correct_kernel,
        out_shape=tuple(f32(3, width) for _ in range(4)),
        in_specs=[VMEM] * 6,
        out_specs=(VMEM,) * 4,
        name="correct",
        **call,
    )(table, parts, *state)


def solution(mesh):
    finer = Mesh(mesh.devices.reshape(8, 4, 12, mesh.shape["rep"]), (Y, X, Z, REP))
    placed = (P(None, BLK), P(None, BLK), P(None, BLK), P(None, BLK), P(BLK), P(BLK, None), P())
    return jax.shard_map(
        shards,
        mesh=finer,
        in_specs=placed,
        out_specs=(P(None, BLK), P(None, BLK), P(None, BLK), P(None, BLK)),
        check_vma=False,
    )
```

```python
import jax
import jax.numpy as jnp
from jax import lax
from jax.experimental import pallas as pl
from jax.experimental.pallas import tpu as pltpu
from jax.sharding import Mesh
from jax.sharding import PartitionSpec as P

Y, X, Z, REP = "blk_0", "blk_1", "blk_2", "rep"
BLK = (Y, X, Z)
FIELD_AXES = (X, Z)
ACT_AXIS = Y

STEP_TIME = 0.0625
SOFTEN_SQ = 0.0001
HALF_SQ = STEP_TIME * STEP_TIME / 2.0
LANES = 128
SLOTS = 16
WIDE = 128
LIMIT = 8 * 1024 * 1024
UNROLL = 24


def lane_iota(shape):
    return lax.broadcasted_iota(jnp.int32, shape, len(shape) - 1)


def row_iota(shape):
    return lax.broadcasted_iota(jnp.int32, shape, len(shape) - 2)


def tiled_slots(index_ref, scratch):
    scratch[...] = jnp.zeros(scratch.shape, jnp.int32)
    scratch[0:1, 0:SLOTS] = index_ref[...]
    row = scratch[0:1, :]
    for shift in (16, 32, 64):
        row = row + pltpu.roll(row, shift, 1)
    return row


def own_rows(shape):
    return row_iota(shape) == lane_iota(shape) // SLOTS


def prepare_kernel(line, *refs):
    given, (field_out, act_out, meta, table) = refs[:7], refs[7:11]
    pos, vel, acc, jerk, mass, index, count, state, slots, tiles, done = refs[11:]
    copies = [
        pltpu.make_async_copy(far, near, done.at[k])
        for k, (far, near) in enumerate(zip(given, (pos, vel, acc, jerk, mass, index, count)))
    ]
    for copy in copies:
        copy.start()
    for copy in copies[:5]:
        copy.wait()
    cubed = STEP_TIME * HALF_SQ / 3.0
    state[0:3, :] = pos[...] + STEP_TIME * vel[...] + HALF_SQ * acc[...] + cubed * jerk[...]
    state[3:6, :] = vel[...] + STEP_TIME * acc[...] + HALF_SQ * jerk[...]
    state[6:7, :] = mass[...]
    state[7:8, :] = jnp.zeros((1, state.shape[1]), jnp.float32)
    whole = state[...]
    half = jnp.where(lax.axis_index(REP) == 0, whole[:, :LANES], whole[:, LANES:])
    for k in range(field_out.shape[0]):
        tiles[k] = half
    sent = pltpu.make_async_copy(tiles, field_out, done.at[7])
    sent.start()
    copies[5].wait()
    shape = (whole.shape[1], LANES)
    tiled = tiled_slots(index, slots)
    chosen = (row_iota(shape) == tiled).astype(jnp.bfloat16)
    picked = jnp.zeros((8, LANES), jnp.float32)
    for part in exact_parts(whole):
        picked = picked + jnp.dot(part, chosen, preferred_element_type=jnp.float32)
    packed = jnp.sum(jnp.where(own_rows(picked.shape), picked, 0.0), axis=0, keepdims=True)
    act_out[...] = packed
    copies[6].wait()
    first, stride = line()
    lane, row = lane_iota((8, LANES)), row_iota((8, LANES))
    known = jnp.zeros((8, LANES), jnp.int32)
    start = 0
    for k in range(lax.axis_size(ACT_AXIS)):
        live = count[first + k * stride]
        known = jnp.where((row == 0) & (lane == k), start, known)
        known = jnp.where((row == 1) & (lane == k), live, known)
        start = start + live
    meta[...] = jnp.where(row == 2, start, known)
    y, x, z = line_base()
    live = count[(y * lax.axis_size(X) + x) * lax.axis_size(Z) + z]
    stars = jnp.broadcast_to(tiled, (8, LANES)).astype(jnp.float32).T[:, 0:1]
    shape = (LANES, table.shape[1])
    here = jnp.broadcast_to(stars, shape) == lane_iota(shape).astype(jnp.float32)
    table[...] = (here & (row_iota(shape) % SLOTS < live)).astype(jnp.bfloat16)
    sent.wait()


def line_base():
    y, x, z = lax.axis_index(Y), lax.axis_index(X), lax.axis_index(Z)
    return y, x, z


def exact_parts(value):
    high = value.astype(jnp.bfloat16)
    rest = value - high.astype(jnp.float32)
    middle = rest.astype(jnp.bfloat16)
    low = (rest - middle.astype(jnp.float32)).astype(jnp.bfloat16)
    return high, middle, low


def spread_kernel(meta, act, active, rows):
    n_line = act.shape[0]
    rows[...] = jnp.zeros(rows.shape, jnp.float32)
    for k in range(n_line):
        rows[k : k + 1, :] = act[k]
    columns = rows[...].T
    lane = lane_iota((1, LANES))
    for k in range(n_line):
        start = jnp.max(jnp.where(lane == k, meta[0:1, :], 0)) if k else 0
        spread = jnp.broadcast_to(columns[0:96, k : k + 1], (96, LANES))
        for c in range(6):
            active[c, pl.ds(start, SLOTS), :] = spread[c * SLOTS : (c + 1) * SLOTS]


def forces_kernel(order, meta, field, active, out, sums, known, done):
    n_line = out.shape[0] // 2
    n_field = field.shape[0]
    copy = pltpu.make_async_copy(meta, known, done)
    copy.start()
    total = jnp.max(meta[2:3, :])

    def one_block(b, carry):
        at = pl.ds(pl.multiple_of(b * 8, 8), 8)
        mine = [active[c, at, :] for c in range(6)]

        def one_chunk(f, sums_here):
            def row(c):
                return jnp.broadcast_to(field[f, c : c + 1, :], (8, LANES))

            dx, dy, dz, du, dv, dw = [row(c) - mine[c] for c in range(6)]
            radius_sq = (dx * dx + dy * dy) + (dz * dz + SOFTEN_SQ)
            root = lax.rsqrt(radius_sq)
            inverse = root * root
            weight = (row(6) * root) * inverse
            radial = (dx * du + dy * dv + dz * dw) * inverse
            wx, wy, wz = weight * dx, weight * dy, weight * dz
            new = (wx, wy, wz, weight * du, weight * dv, weight * dw, radial * wx, radial * wy, radial * wz)
            return tuple(s + n for s, n in zip(sums_here, new))

        zero = jnp.zeros((8, LANES), jnp.float32)
        got = lax.fori_loop(0, n_field, one_chunk, (zero,) * 9, unroll=UNROLL)
        for c in range(3):
            sums[c, at, :] = got[c]
            sums[3 + c, at, :] = got[3 + c] - 3.0 * got[6 + c]
        return carry

    lax.fori_loop(0, (total + 7) // 8, one_block, 0)
    folded = jnp.zeros((8, WIDE), jnp.float32)
    for c in range(6):
        ones = (row_iota((8, LANES)) == c).astype(jnp.bfloat16)
        row = jnp.zeros((8, WIDE), jnp.float32)
        for part in exact_parts(sums[c]):
            row = row + lax.dot_general(ones, part, (((1,), (1,)), ((), ())), preferred_element_type=jnp.float32)
        row = jnp.where(row_iota((8, WIDE)) == c, row, 0.0)
        folded = folded + (pltpu.roll(row, SLOTS * c, 1) if c else row)
    lane = lane_iota((8, LANES))
    owned = own_rows((8, LANES))
    copy.wait()
    for k in range(n_line):
        moved = pltpu.roll(folded, WIDE - known[0, k], 1) if k else folded
        kept = jnp.where(owned & (lane % SLOTS < known[1, k]), moved, 0.0)
        packed = jnp.sum(kept, axis=0, keepdims=True)
        for j, member in enumerate(order):
            if member // 2 == k:
                out[j] = packed


def correct_kernel(table, parts, pos, vel, acc, jerk, new_pos, new_vel, new_acc, new_jerk):
    force = parts[0]
    for k in range(1, parts.shape[0]):
        force = force + parts[k]
    shape = (8, LANES)
    spread = jnp.where(own_rows(shape), jnp.broadcast_to(force, shape), 0.0)
    spread = jnp.where((row_iota(shape) == 6) & own_rows(shape), 1.0, spread)
    placed = jnp.zeros((8, table.shape[1]), jnp.float32)
    for part in exact_parts(spread):
        placed = placed + jnp.dot(part, table[...], preferred_element_type=jnp.float32)
    hit = jnp.broadcast_to(placed[6:7], (3, placed.shape[1])) > 0.5
    acc_one, jerk_one = placed[0:3], placed[3:6]
    pos_zero, vel_zero, acc_zero, jerk_zero = pos[...], vel[...], acc[...], jerk[...]
    twelfth = STEP_TIME * STEP_TIME / 12.0
    vel_one = vel_zero + (acc_zero + acc_one) * (STEP_TIME / 2.0) + (jerk_zero - jerk_one) * twelfth
    pos_one = pos_zero + (vel_zero + vel_one) * (STEP_TIME / 2.0) + (acc_zero - acc_one) * twelfth
    new_pos[...] = jnp.where(hit, pos_one, pos_zero)
    new_vel[...] = jnp.where(hit, vel_one, vel_zero)
    new_acc[...] = jnp.where(hit, acc_one, acc_zero)
    new_jerk[...] = jnp.where(hit, jerk_one, jerk_zero)


def f32(*shape):
    return jax.ShapeDtypeStruct(shape, jnp.float32)


VMEM = pl.BlockSpec(memory_space=pltpu.VMEM)
HBM = pl.BlockSpec(memory_space=pltpu.HBM)


def shards(star_pos, star_vel, star_acc, star_jerk, masses, act_index, act_count):
    n_field = lax.axis_size(FIELD_AXES)
    n_line = lax.axis_size(ACT_AXIS)
    state = (star_pos, star_vel, star_acc, star_jerk)
    width = star_pos.shape[1]

    def line():
        y, x, z = line_base()
        return x * lax.axis_size(Z) + z, lax.axis_size(X) * lax.axis_size(Z)

    given = (*state, masses[None, :], act_index, act_count)
    call = dict(compiler_params=pltpu.CompilerParams(vmem_limit_bytes=LIMIT))
    field, act, meta, table = pl.pallas_call(
        lambda *refs: prepare_kernel(line, *refs),
        out_shape=(
            pltpu.HBM((n_field, 8, LANES), jnp.float32),
            pltpu.VMEM((1, LANES), jnp.float32),
            pltpu.VMEM((8, LANES), jnp.int32),
            pltpu.VMEM((LANES, width), jnp.bfloat16),
        ),
        in_specs=[HBM] * 7,
        out_specs=(HBM, VMEM, VMEM, VMEM),
        scratch_shapes=[pltpu.VMEM((3, width), jnp.float32)] * 4
        + [
            pltpu.VMEM((1, width), jnp.float32),
            pltpu.VMEM((1, SLOTS), jnp.int32),
            pltpu.SMEM(act_count.shape, jnp.int32),
            pltpu.VMEM((8, width), jnp.float32),
            pltpu.VMEM((8, LANES), jnp.int32),
            pltpu.VMEM((n_field, 8, LANES), jnp.float32),
            pltpu.SemaphoreType.DMA((8,)),
        ],
        name="prepare",
        **call,
    )(*[pltpu.with_memory_space_constraint(a, pltpu.HBM) for a in given])
    field = lax.all_to_all(field, FIELD_AXES, 0, 0, tiled=True)
    act = lax.all_gather(act, ACT_AXIS)
    active = pl.pallas_call(
        spread_kernel,
        out_shape=pltpu.VMEM((6, WIDE + SLOTS, LANES), jnp.float32),
        in_specs=[VMEM] * 2,
        out_specs=VMEM,
        scratch_shapes=[pltpu.VMEM((8, LANES), jnp.float32)],
        name="spread",
        **call,
    )(meta, act)
    order = [2 * ((j // 2 + n_line // 2) % n_line) + 1 - j % 2 for j in range(2 * n_line)]
    parts = pl.pallas_call(
        lambda *refs: forces_kernel(order, *refs),
        out_shape=pltpu.VMEM((2 * n_line, 1, LANES), jnp.float32),
        in_specs=[VMEM] * 3,
        out_specs=VMEM,
        scratch_shapes=[
            pltpu.VMEM((6, WIDE, LANES), jnp.float32),
            pltpu.SMEM((8, LANES), jnp.int32),
            pltpu.SemaphoreType.DMA(()),
        ],
        name="forces",
        **call,
    )(meta, field, active)
    parts = lax.all_to_all(parts, (ACT_AXIS, REP), 0, 0, axis_index_groups=[order], tiled=True)
    return pl.pallas_call(
        correct_kernel,
        out_shape=tuple(f32(3, width) for _ in range(4)),
        in_specs=[VMEM] * 6,
        out_specs=(VMEM,) * 4,
        name="correct",
        **call,
    )(table, parts, *state)


def solution(mesh):
    finer = Mesh(mesh.devices.reshape(8, 4, 12, mesh.shape["rep"]), (Y, X, Z, REP))
    placed = (P(None, BLK), P(None, BLK), P(None, BLK), P(None, BLK), P(BLK), P(BLK, None), P())
    return jax.shard_map(
        shards,
        mesh=finer,
        in_specs=placed,
        out_specs=(P(None, BLK), P(None, BLK), P(None, BLK), P(None, BLK)),
        check_vma=False,
    )
```

```python
import jax
import jax.numpy as jnp
from jax import lax
from jax.experimental import pallas as pl
from jax.experimental.pallas import tpu as pltpu
from jax.sharding import Mesh
from jax.sharding import PartitionSpec as P

Y, X, Z, REP = "blk_0", "blk_1", "blk_2", "rep"
BLK = (Y, X, Z)
FIELD_AXES = (X, Z)
ACT_AXIS = Y

STEP_TIME = 0.0625
SOFTEN_SQ = 0.0001
HALF_SQ = STEP_TIME * STEP_TIME / 2.0
LANES = 128
SLOTS = 16
WIDE = 128
LIMIT = 8 * 1024 * 1024
UNROLL = 24


def lane_iota(shape):
    return lax.broadcasted_iota(jnp.int32, shape, len(shape) - 1)


def row_iota(shape):
    return lax.broadcasted_iota(jnp.int32, shape, len(shape) - 2)


def tiled_slots(index_ref, scratch):
    scratch[...] = jnp.zeros(scratch.shape, jnp.int32)
    scratch[0:1, 0:SLOTS] = index_ref[...]
    row = scratch[0:1, :]
    for shift in (16, 32, 64):
        row = row + pltpu.roll(row, shift, 1)
    return row


def own_rows(shape):
    return row_iota(shape) == lane_iota(shape) // SLOTS


def prepare_kernel(line, *refs):
    given, (field_out, act_out, meta, table) = refs[:7], refs[7:11]
    pos, vel, acc, jerk, mass, index, count, state, slots, done = refs[11:]
    copies = [
        pltpu.make_async_copy(far, near, done.at[k])
        for k, (far, near) in enumerate(zip(given, (pos, vel, acc, jerk, mass, index, count)))
    ]
    for copy in copies:
        copy.start()
    for copy in copies:
        copy.wait()
    cubed = STEP_TIME * HALF_SQ / 3.0
    state[0:3, :] = pos[...] + STEP_TIME * vel[...] + HALF_SQ * acc[...] + cubed * jerk[...]
    state[3:6, :] = vel[...] + STEP_TIME * acc[...] + HALF_SQ * jerk[...]
    state[6:7, :] = mass[...]
    state[7:8, :] = jnp.zeros((1, state.shape[1]), jnp.float32)
    whole = state[...]
    half = jnp.where(lax.axis_index(REP) == 0, whole[:, :LANES], whole[:, LANES:])
    for k in range(field_out.shape[0]):
        field_out[k] = half
    shape = (whole.shape[1], LANES)
    tiled = tiled_slots(index, slots)
    chosen = (row_iota(shape) == tiled).astype(jnp.bfloat16)
    picked = jnp.zeros((8, LANES), jnp.float32)
    for part in exact_parts(whole):
        picked = picked + jnp.dot(part, chosen, preferred_element_type=jnp.float32)
    packed = jnp.sum(jnp.where(own_rows(picked.shape), picked, 0.0), axis=0, keepdims=True)
    act_out[...] = packed
    first, stride = line()
    lane, row = lane_iota((8, LANES)), row_iota((8, LANES))
    known = jnp.zeros((8, LANES), jnp.int32)
    start = 0
    for k in range(lax.axis_size(ACT_AXIS)):
        live = count[first + k * stride]
        known = jnp.where((row == 0) & (lane == k), start, known)
        known = jnp.where((row == 1) & (lane == k), live, known)
        start = start + live
    meta[...] = jnp.where(row == 2, start, known)
    y, x, z = line_base()
    live = count[(y * lax.axis_size(X) + x) * lax.axis_size(Z) + z]
    stars = jnp.broadcast_to(tiled, (8, LANES)).astype(jnp.float32).T[:, 0:1]
    shape = (LANES, table.shape[1])
    here = jnp.broadcast_to(stars, shape) == lane_iota(shape).astype(jnp.float32)
    table[...] = (here & (row_iota(shape) % SLOTS < live)).astype(jnp.bfloat16)


def line_base():
    y, x, z = lax.axis_index(Y), lax.axis_index(X), lax.axis_index(Z)
    return y, x, z


def exact_parts(value):
    high = value.astype(jnp.bfloat16)
    rest = value - high.astype(jnp.float32)
    middle = rest.astype(jnp.bfloat16)
    low = (rest - middle.astype(jnp.float32)).astype(jnp.bfloat16)
    return high, middle, low


def spread_kernel(meta, act, active, rows):
    n_line = act.shape[0]
    rows[...] = jnp.zeros(rows.shape, jnp.float32)
    for k in range(n_line):
        rows[k : k + 1, :] = act[k]
    columns = rows[...].T
    lane = lane_iota((1, LANES))
    for k in range(n_line):
        start = jnp.max(jnp.where(lane == k, meta[0:1, :], 0)) if k else 0
        spread = jnp.broadcast_to(columns[0:96, k : k + 1], (96, LANES))
        for c in range(6):
            active[c, pl.ds(start, SLOTS), :] = spread[c * SLOTS : (c + 1) * SLOTS]


def forces_kernel(order, meta, field, active, out, sums, known, done):
    n_line = out.shape[0] // 2
    n_field = field.shape[0]
    copy = pltpu.make_async_copy(meta, known, done)
    copy.start()
    total = jnp.max(meta[2:3, :])

    def one_block(b, carry):
        at = pl.ds(pl.multiple_of(b * 8, 8), 8)
        mine = [active[c, at, :] for c in range(6)]

        def one_chunk(f, sums_here):
            def row(c):
                return jnp.broadcast_to(field[f, c : c + 1, :], (8, LANES))

            dx, dy, dz, du, dv, dw = [row(c) - mine[c] for c in range(6)]
            radius_sq = (dx * dx + dy * dy) + (dz * dz + SOFTEN_SQ)
            root = lax.rsqrt(radius_sq)
            inverse = root * root
            weight = (row(6) * root) * inverse
            radial = (dx * du + dy * dv + dz * dw) * inverse
            wx, wy, wz = weight * dx, weight * dy, weight * dz
            new = (wx, wy, wz, weight * du, weight * dv, weight * dw, radial * wx, radial * wy, radial * wz)
            return tuple(s + n for s, n in zip(sums_here, new))

        zero = jnp.zeros((8, LANES), jnp.float32)
        got = lax.fori_loop(0, n_field, one_chunk, (zero,) * 9, unroll=UNROLL)
        for c in range(3):
            sums[c, at, :] = got[c]
            sums[3 + c, at, :] = got[3 + c] - 3.0 * got[6 + c]
        return carry

    lax.fori_loop(0, (total + 7) // 8, one_block, 0)
    folded = jnp.zeros((8, WIDE), jnp.float32)
    for c in range(6):
        ones = (row_iota((8, LANES)) == c).astype(jnp.bfloat16)
        row = jnp.zeros((8, WIDE), jnp.float32)
        for part in exact_parts(sums[c]):
            row = row + lax.dot_general(ones, part, (((1,), (1,)), ((), ())), preferred_element_type=jnp.float32)
        row = jnp.where(row_iota((8, WIDE)) == c, row, 0.0)
        folded = folded + (pltpu.roll(row, SLOTS * c, 1) if c else row)
    lane = lane_iota((8, LANES))
    owned = own_rows((8, LANES))
    copy.wait()
    for k in range(n_line):
        moved = pltpu.roll(folded, WIDE - known[0, k], 1) if k else folded
        kept = jnp.where(owned & (lane % SLOTS < known[1, k]), moved, 0.0)
        packed = jnp.sum(kept, axis=0, keepdims=True)
        for j, member in enumerate(order):
            if member // 2 == k:
                out[j] = packed


def correct_kernel(table, parts, pos, vel, acc, jerk, new_pos, new_vel, new_acc, new_jerk):
    force = parts[0]
    for k in range(1, parts.shape[0]):
        force = force + parts[k]
    shape = (8, LANES)
    spread = jnp.where(own_rows(shape), jnp.broadcast_to(force, shape), 0.0)
    spread = jnp.where((row_iota(shape) == 6) & own_rows(shape), 1.0, spread)
    placed = jnp.zeros((8, table.shape[1]), jnp.float32)
    for part in exact_parts(spread):
        placed = placed + jnp.dot(part, table[...], preferred_element_type=jnp.float32)
    hit = jnp.broadcast_to(placed[6:7], (3, placed.shape[1])) > 0.5
    acc_one, jerk_one = placed[0:3], placed[3:6]
    pos_zero, vel_zero, acc_zero, jerk_zero = pos[...], vel[...], acc[...], jerk[...]
    twelfth = STEP_TIME * STEP_TIME / 12.0
    vel_one = vel_zero + (acc_zero + acc_one) * (STEP_TIME / 2.0) + (jerk_zero - jerk_one) * twelfth
    pos_one = pos_zero + (vel_zero + vel_one) * (STEP_TIME / 2.0) + (acc_zero - acc_one) * twelfth
    new_pos[...] = jnp.where(hit, pos_one, pos_zero)
    new_vel[...] = jnp.where(hit, vel_one, vel_zero)
    new_acc[...] = jnp.where(hit, acc_one, acc_zero)
    new_jerk[...] = jnp.where(hit, jerk_one, jerk_zero)


def f32(*shape):
    return jax.ShapeDtypeStruct(shape, jnp.float32)


VMEM = pl.BlockSpec(memory_space=pltpu.VMEM)
HBM = pl.BlockSpec(memory_space=pltpu.HBM)


def shards(star_pos, star_vel, star_acc, star_jerk, masses, act_index, act_count):
    n_field = lax.axis_size(FIELD_AXES)
    n_line = lax.axis_size(ACT_AXIS)
    state = (star_pos, star_vel, star_acc, star_jerk)
    width = star_pos.shape[1]

    def line():
        y, x, z = line_base()
        return x * lax.axis_size(Z) + z, lax.axis_size(X) * lax.axis_size(Z)

    given = (*state, masses[None, :], act_index, act_count)
    call = dict(compiler_params=pltpu.CompilerParams(vmem_limit_bytes=LIMIT))
    field, act, meta, table = pl.pallas_call(
        lambda *refs: prepare_kernel(line, *refs),
        out_shape=(
            pltpu.VMEM((n_field, 8, LANES), jnp.float32),
            pltpu.VMEM((1, LANES), jnp.float32),
            pltpu.VMEM((8, LANES), jnp.int32),
            pltpu.VMEM((LANES, width), jnp.bfloat16),
        ),
        in_specs=[HBM] * 7,
        out_specs=(VMEM,) * 4,
        scratch_shapes=[pltpu.VMEM((3, width), jnp.float32)] * 4
        + [
            pltpu.VMEM((1, width), jnp.float32),
            pltpu.VMEM((1, SLOTS), jnp.int32),
            pltpu.SMEM(act_count.shape, jnp.int32),
            pltpu.VMEM((8, width), jnp.float32),
            pltpu.VMEM((8, LANES), jnp.int32),
            pltpu.SemaphoreType.DMA((7,)),
        ],
        name="prepare",
        **call,
    )(*[pltpu.with_memory_space_constraint(a, pltpu.HBM) for a in given])
    field = lax.all_to_all(field, FIELD_AXES, 0, 0, tiled=True)
    act = lax.all_gather(act, ACT_AXIS)
    active = pl.pallas_call(
        spread_kernel,
        out_shape=pltpu.VMEM((6, WIDE + SLOTS, LANES), jnp.float32),
        in_specs=[VMEM] * 2,
        out_specs=VMEM,
        scratch_shapes=[pltpu.VMEM((8, LANES), jnp.float32)],
        name="spread",
        **call,
    )(meta, act)
    order = [2 * ((j // 2 + n_line // 2) % n_line) + 1 - j % 2 for j in range(2 * n_line)]
    parts = pl.pallas_call(
        lambda *refs: forces_kernel(order, *refs),
        out_shape=pltpu.VMEM((2 * n_line, 1, LANES), jnp.float32),
        in_specs=[VMEM] * 3,
        out_specs=VMEM,
        scratch_shapes=[
            pltpu.VMEM((6, WIDE, LANES), jnp.float32),
            pltpu.SMEM((8, LANES), jnp.int32),
            pltpu.SemaphoreType.DMA(()),
        ],
        name="forces",
        **call,
    )(meta, field, active)
    parts = lax.all_to_all(parts, (ACT_AXIS, REP), 0, 0, axis_index_groups=[order], tiled=True)
    return pl.pallas_call(
        correct_kernel,
        out_shape=tuple(f32(3, width) for _ in range(4)),
        in_specs=[VMEM] * 6,
        out_specs=(VMEM,) * 4,
        name="correct",
        **call,
    )(table, parts, *state)


def solution(mesh):
    finer = Mesh(mesh.devices.reshape(8, 4, 12, mesh.shape["rep"]), (Y, X, Z, REP))
    placed = (P(None, BLK), P(None, BLK), P(None, BLK), P(None, BLK), P(BLK), P(BLK, None), P())
    return jax.shard_map(
        shards,
        mesh=finer,
        in_specs=placed,
        out_specs=(P(None, BLK), P(None, BLK), P(None, BLK), P(None, BLK)),
        check_vma=False,
    )
```

```python
import jax
import jax.numpy as jnp
from jax import lax
from jax.experimental import pallas as pl
from jax.experimental.pallas import tpu as pltpu
from jax.sharding import Mesh
from jax.sharding import PartitionSpec as P

Y, X, Z, REP = "blk_0", "blk_1", "blk_2", "rep"
BLK = (Y, X, Z)
FIELD_AXES = (X, Z)
ACT_AXIS = Y

STEP_TIME = 0.0625
SOFTEN_SQ = 0.0001
HALF_SQ = STEP_TIME * STEP_TIME / 2.0
LANES = 128
SLOTS = 16
WIDE = 128
LIMIT = 8 * 1024 * 1024
UNROLL = 24


def lane_iota(shape):
    return lax.broadcasted_iota(jnp.int32, shape, len(shape) - 1)


def row_iota(shape):
    return lax.broadcasted_iota(jnp.int32, shape, len(shape) - 2)


def tiled_slots(index_ref, scratch):
    scratch[...] = jnp.zeros(scratch.shape, jnp.int32)
    scratch[0:1, 0:SLOTS] = index_ref[...]
    row = scratch[0:1, :]
    for shift in (16, 32, 64):
        row = row + pltpu.roll(row, shift, 1)
    return row


def own_rows(shape):
    return row_iota(shape) == lane_iota(shape) // SLOTS


def prepare_kernel(line, *refs):
    given, (field_out, act_out, meta, table) = refs[:7], refs[7:11]
    pos, vel, acc, jerk, mass, index, count, state, slots, done = refs[11:]
    copies = [
        pltpu.make_async_copy(far, near, done.at[k])
        for k, (far, near) in enumerate(zip(given, (pos, vel, acc, jerk, mass, index, count)))
    ]
    for copy in copies:
        copy.start()
    for copy in copies[:5]:
        copy.wait()
    cubed = STEP_TIME * HALF_SQ / 3.0
    state[0:3, :] = pos[...] + STEP_TIME * vel[...] + HALF_SQ * acc[...] + cubed * jerk[...]
    state[3:6, :] = vel[...] + STEP_TIME * acc[...] + HALF_SQ * jerk[...]
    state[6:7, :] = mass[...]
    state[7:8, :] = jnp.zeros((1, state.shape[1]), jnp.float32)
    whole = state[...]
    half = jnp.where(lax.axis_index(REP) == 0, whole[:, :LANES], whole[:, LANES:])
    for k in range(field_out.shape[0]):
        field_out[k] = half
    shape = (whole.shape[1], LANES)
    copies[5].wait()
    tiled = tiled_slots(index, slots)
    chosen = (row_iota(shape) == tiled).astype(jnp.bfloat16)
    picked = jnp.zeros((8, LANES), jnp.float32)
    for part in exact_parts(whole):
        picked = picked + jnp.dot(part, chosen, preferred_element_type=jnp.float32)
    packed = jnp.sum(jnp.where(own_rows(picked.shape), picked, 0.0), axis=0, keepdims=True)
    act_out[...] = packed
    copies[6].wait()
    first, stride = line()
    lane, row = lane_iota((8, LANES)), row_iota((8, LANES))
    known = jnp.zeros((8, LANES), jnp.int32)
    start = 0
    for k in range(lax.axis_size(ACT_AXIS)):
        live = count[first + k * stride]
        known = jnp.where((row == 0) & (lane == k), start, known)
        known = jnp.where((row == 1) & (lane == k), live, known)
        start = start + live
    meta[...] = jnp.where(row == 2, start, known)
    y, x, z = line_base()
    live = count[(y * lax.axis_size(X) + x) * lax.axis_size(Z) + z]
    stars = jnp.broadcast_to(tiled, (8, LANES)).astype(jnp.float32).T[:, 0:1]
    shape = (LANES, table.shape[1])
    here = jnp.broadcast_to(stars, shape) == lane_iota(shape).astype(jnp.float32)
    table[...] = (here & (row_iota(shape) % SLOTS < live)).astype(jnp.bfloat16)


def line_base():
    y, x, z = lax.axis_index(Y), lax.axis_index(X), lax.axis_index(Z)
    return y, x, z


def exact_parts(value):
    high = value.astype(jnp.bfloat16)
    rest = value - high.astype(jnp.float32)
    middle = rest.astype(jnp.bfloat16)
    low = (rest - middle.astype(jnp.float32)).astype(jnp.bfloat16)
    return high, middle, low


def spread_kernel(meta, act, active, rows):
    n_line = act.shape[0]
    rows[...] = jnp.zeros(rows.shape, jnp.float32)
    for k in range(n_line):
        rows[k : k + 1, :] = act[k]
    columns = rows[...].T
    lane = lane_iota((1, LANES))
    for k in range(n_line):
        start = jnp.max(jnp.where(lane == k, meta[0:1, :], 0)) if k else 0
        spread = jnp.broadcast_to(columns[0:96, k : k + 1], (96, LANES))
        for c in range(6):
            active[c, pl.ds(start, SLOTS), :] = spread[c * SLOTS : (c + 1) * SLOTS]


def forces_kernel(order, meta, field, active, out, sums, known, done):
    n_line = out.shape[0] // 2
    n_field = field.shape[0]
    copy = pltpu.make_async_copy(meta, known, done)
    copy.start()
    total = jnp.max(meta[2:3, :])

    def one_block(b, carry):
        at = pl.ds(pl.multiple_of(b * 8, 8), 8)
        mine = [active[c, at, :] for c in range(6)]

        def one_chunk(f, sums_here):
            def row(c):
                return jnp.broadcast_to(field[f, c : c + 1, :], (8, LANES))

            dx, dy, dz, du, dv, dw = [row(c) - mine[c] for c in range(6)]
            radius_sq = (dx * dx + dy * dy) + (dz * dz + SOFTEN_SQ)
            root = lax.rsqrt(radius_sq)
            inverse = root * root
            weight = (row(6) * root) * inverse
            radial = (dx * du + dy * dv + dz * dw) * inverse
            wx, wy, wz = weight * dx, weight * dy, weight * dz
            new = (wx, wy, wz, weight * du, weight * dv, weight * dw, radial * wx, radial * wy, radial * wz)
            return tuple(s + n for s, n in zip(sums_here, new))

        zero = jnp.zeros((8, LANES), jnp.float32)
        got = lax.fori_loop(0, n_field, one_chunk, (zero,) * 9, unroll=UNROLL)
        for c in range(3):
            sums[c, at, :] = got[c]
            sums[3 + c, at, :] = got[3 + c] - 3.0 * got[6 + c]
        return carry

    lax.fori_loop(0, (total + 7) // 8, one_block, 0)
    folded = jnp.zeros((8, WIDE), jnp.float32)
    for c in range(6):
        ones = (row_iota((8, LANES)) == c).astype(jnp.bfloat16)
        row = jnp.zeros((8, WIDE), jnp.float32)
        for part in exact_parts(sums[c]):
            row = row + lax.dot_general(ones, part, (((1,), (1,)), ((), ())), preferred_element_type=jnp.float32)
        row = jnp.where(row_iota((8, WIDE)) == c, row, 0.0)
        folded = folded + (pltpu.roll(row, SLOTS * c, 1) if c else row)
    lane = lane_iota((8, LANES))
    owned = own_rows((8, LANES))
    copy.wait()
    for k in range(n_line):
        moved = pltpu.roll(folded, WIDE - known[0, k], 1) if k else folded
        kept = jnp.where(owned & (lane % SLOTS < known[1, k]), moved, 0.0)
        packed = jnp.sum(kept, axis=0, keepdims=True)
        for j, member in enumerate(order):
            if member // 2 == k:
                out[j] = packed


def correct_kernel(table, parts, pos, vel, acc, jerk, new_pos, new_vel, new_acc, new_jerk):
    force = parts[0]
    for k in range(1, parts.shape[0]):
        force = force + parts[k]
    shape = (8, LANES)
    spread = jnp.where(own_rows(shape), jnp.broadcast_to(force, shape), 0.0)
    spread = jnp.where((row_iota(shape) == 6) & own_rows(shape), 1.0, spread)
    placed = jnp.zeros((8, table.shape[1]), jnp.float32)
    for part in exact_parts(spread):
        placed = placed + jnp.dot(part, table[...], preferred_element_type=jnp.float32)
    hit = jnp.broadcast_to(placed[6:7], (3, placed.shape[1])) > 0.5
    acc_one, jerk_one = placed[0:3], placed[3:6]
    pos_zero, vel_zero, acc_zero, jerk_zero = pos[...], vel[...], acc[...], jerk[...]
    twelfth = STEP_TIME * STEP_TIME / 12.0
    vel_one = vel_zero + (acc_zero + acc_one) * (STEP_TIME / 2.0) + (jerk_zero - jerk_one) * twelfth
    pos_one = pos_zero + (vel_zero + vel_one) * (STEP_TIME / 2.0) + (acc_zero - acc_one) * twelfth
    new_pos[...] = jnp.where(hit, pos_one, pos_zero)
    new_vel[...] = jnp.where(hit, vel_one, vel_zero)
    new_acc[...] = jnp.where(hit, acc_one, acc_zero)
    new_jerk[...] = jnp.where(hit, jerk_one, jerk_zero)


def f32(*shape):
    return jax.ShapeDtypeStruct(shape, jnp.float32)


VMEM = pl.BlockSpec(memory_space=pltpu.VMEM)
HBM = pl.BlockSpec(memory_space=pltpu.HBM)


def shards(star_pos, star_vel, star_acc, star_jerk, masses, act_index, act_count):
    n_field = lax.axis_size(FIELD_AXES)
    n_line = lax.axis_size(ACT_AXIS)
    state = (star_pos, star_vel, star_acc, star_jerk)
    width = star_pos.shape[1]

    def line():
        y, x, z = line_base()
        return x * lax.axis_size(Z) + z, lax.axis_size(X) * lax.axis_size(Z)

    given = (*state, masses[None, :], act_index, act_count)
    call = dict(compiler_params=pltpu.CompilerParams(vmem_limit_bytes=LIMIT))
    field, act, meta, table = pl.pallas_call(
        lambda *refs: prepare_kernel(line, *refs),
        out_shape=(
            pltpu.VMEM((n_field, 8, LANES), jnp.float32),
            pltpu.VMEM((1, LANES), jnp.float32),
            pltpu.VMEM((8, LANES), jnp.int32),
            pltpu.VMEM((LANES, width), jnp.bfloat16),
        ),
        in_specs=[HBM] * 7,
        out_specs=(VMEM,) * 4,
        scratch_shapes=[pltpu.VMEM((3, width), jnp.float32)] * 4
        + [
            pltpu.VMEM((1, width), jnp.float32),
            pltpu.VMEM((1, SLOTS), jnp.int32),
            pltpu.SMEM(act_count.shape, jnp.int32),
            pltpu.VMEM((8, width), jnp.float32),
            pltpu.VMEM((8, LANES), jnp.int32),
            pltpu.SemaphoreType.DMA((7,)),
        ],
        name="prepare",
        **call,
    )(*[pltpu.with_memory_space_constraint(a, pltpu.HBM) for a in given])
    field = lax.all_to_all(field, FIELD_AXES, 0, 0, tiled=True)
    act = lax.all_gather(act, ACT_AXIS)
    active = pl.pallas_call(
        spread_kernel,
        out_shape=pltpu.VMEM((6, WIDE + SLOTS, LANES), jnp.float32),
        in_specs=[VMEM] * 2,
        out_specs=VMEM,
        scratch_shapes=[pltpu.VMEM((8, LANES), jnp.float32)],
        name="spread",
        **call,
    )(meta, act)
    order = [2 * ((j // 2 + n_line // 2) % n_line) + 1 - j % 2 for j in range(2 * n_line)]
    parts = pl.pallas_call(
        lambda *refs: forces_kernel(order, *refs),
        out_shape=pltpu.VMEM((2 * n_line, 1, LANES), jnp.float32),
        in_specs=[VMEM] * 3,
        out_specs=VMEM,
        scratch_shapes=[
            pltpu.VMEM((6, WIDE, LANES), jnp.float32),
            pltpu.SMEM((8, LANES), jnp.int32),
            pltpu.SemaphoreType.DMA(()),
        ],
        name="forces",
        **call,
    )(meta, field, active)
    parts = lax.all_to_all(parts, (ACT_AXIS, REP), 0, 0, axis_index_groups=[order], tiled=True)
    return pl.pallas_call(
        correct_kernel,
        out_shape=tuple(f32(3, width) for _ in range(4)),
        in_specs=[VMEM] * 6,
        out_specs=(VMEM,) * 4,
        name="correct",
        **call,
    )(table, parts, *state)


def solution(mesh):
    finer = Mesh(mesh.devices.reshape(8, 4, 12, mesh.shape["rep"]), (Y, X, Z, REP))
    placed = (P(None, BLK), P(None, BLK), P(None, BLK), P(None, BLK), P(BLK), P(BLK, None), P())
    return jax.shard_map(
        shards,
        mesh=finer,
        in_specs=placed,
        out_specs=(P(None, BLK), P(None, BLK), P(None, BLK), P(None, BLK)),
        check_vma=False,
    )
```

```python
import jax
import jax.numpy as jnp
from jax import lax
from jax.experimental import pallas as pl
from jax.experimental.pallas import tpu as pltpu
from jax.sharding import Mesh
from jax.sharding import PartitionSpec as P

Y, X, Z, REP = "blk_0", "blk_1", "blk_2", "rep"
BLK = (Y, X, Z)
FIELD_AXES = (X, Z)
ACT_AXIS = Y

STEP_TIME = 0.0625
SOFTEN_SQ = 0.0001
HALF_SQ = STEP_TIME * STEP_TIME / 2.0
LANES = 128
SLOTS = 16
WIDE = 128
LIMIT = 8 * 1024 * 1024
UNROLL = 24


def lane_iota(shape):
    return lax.broadcasted_iota(jnp.int32, shape, len(shape) - 1)


def row_iota(shape):
    return lax.broadcasted_iota(jnp.int32, shape, len(shape) - 2)


def tiled_slots(index_ref, scratch):
    scratch[...] = jnp.zeros(scratch.shape, jnp.int32)
    scratch[0:1, 0:SLOTS] = index_ref[...]
    row = scratch[0:1, :]
    for shift in (16, 32, 64):
        row = row + pltpu.roll(row, shift, 1)
    return row


def own_rows(shape):
    return row_iota(shape) == lane_iota(shape) // SLOTS


def prepare_kernel(line, *refs):
    given, (field_out, act_out, meta, table) = refs[:7], refs[7:11]
    pos, vel, acc, jerk, mass, index, count, state, slots, done = refs[11:]
    copies = [
        pltpu.make_async_copy(far, near, done.at[k])
        for k, (far, near) in enumerate(zip(given, (pos, vel, acc, jerk, mass, index, count)))
    ]
    for copy in copies:
        copy.start()
    for copy in copies[:5]:
        copy.wait()
    cubed = STEP_TIME * HALF_SQ / 3.0
    state[0:3, :] = pos[...] + STEP_TIME * vel[...] + HALF_SQ * acc[...] + cubed * jerk[...]
    state[3:6, :] = vel[...] + STEP_TIME * acc[...] + HALF_SQ * jerk[...]
    state[6:7, :] = mass[...]
    state[7:8, :] = jnp.zeros((1, state.shape[1]), jnp.float32)
    whole = state[...]
    half = jnp.where(lax.axis_index(REP) == 0, whole[:7, :LANES], whole[:7, LANES:])
    for k in range(field_out.shape[0]):
        field_out[k] = half
    shape = (whole.shape[1], LANES)
    copies[5].wait()
    tiled = tiled_slots(index, slots)
    chosen = (row_iota(shape) == tiled).astype(jnp.bfloat16)
    picked = jnp.zeros((8, LANES), jnp.float32)
    for part in exact_parts(whole):
        picked = picked + jnp.dot(part, chosen, preferred_element_type=jnp.float32)
    packed = jnp.sum(jnp.where(own_rows(picked.shape), picked, 0.0), axis=0, keepdims=True)
    act_out[...] = packed
    copies[6].wait()
    first, stride = line()
    lane, row = lane_iota((8, LANES)), row_iota((8, LANES))
    known = jnp.zeros((8, LANES), jnp.int32)
    start = 0
    for k in range(lax.axis_size(ACT_AXIS)):
        live = count[first + k * stride]
        known = jnp.where((row == 0) & (lane == k), start, known)
        known = jnp.where((row == 1) & (lane == k), live, known)
        start = start + live
    meta[...] = jnp.where(row == 2, start, known)
    y, x, z = line_base()
    live = count[(y * lax.axis_size(X) + x) * lax.axis_size(Z) + z]
    stars = jnp.broadcast_to(tiled, (8, LANES)).astype(jnp.float32).T[:, 0:1]
    shape = (LANES, table.shape[1])
    here = jnp.broadcast_to(stars, shape) == lane_iota(shape).astype(jnp.float32)
    table[...] = (here & (row_iota(shape) % SLOTS < live)).astype(jnp.bfloat16)


def line_base():
    y, x, z = lax.axis_index(Y), lax.axis_index(X), lax.axis_index(Z)
    return y, x, z


def exact_parts(value):
    high = value.astype(jnp.bfloat16)
    rest = value - high.astype(jnp.float32)
    middle = rest.astype(jnp.bfloat16)
    low = (rest - middle.astype(jnp.float32)).astype(jnp.bfloat16)
    return high, middle, low


def spread_kernel(meta, act, active, rows):
    n_line = act.shape[0]
    rows[...] = jnp.zeros(rows.shape, jnp.float32)
    for k in range(n_line):
        rows[k : k + 1, :] = act[k]
    columns = rows[...].T
    lane = lane_iota((1, LANES))
    for k in range(n_line):
        start = jnp.max(jnp.where(lane == k, meta[0:1, :], 0)) if k else 0
        spread = jnp.broadcast_to(columns[0:96, k : k + 1], (96, LANES))
        for c in range(6):
            active[c, pl.ds(start, SLOTS), :] = spread[c * SLOTS : (c + 1) * SLOTS]


def forces_kernel(order, meta, field, active, out, sums, known, done):
    n_line = out.shape[0] // 2
    n_field = field.shape[0]
    copy = pltpu.make_async_copy(meta, known, done)
    copy.start()
    total = jnp.max(meta[2:3, :])

    def one_block(b, carry):
        at = pl.ds(pl.multiple_of(b * 8, 8), 8)
        mine = [active[c, at, :] for c in range(6)]

        def one_chunk(f, sums_here):
            def row(c):
                return jnp.broadcast_to(field[f, c : c + 1, :], (8, LANES))

            dx, dy, dz, du, dv, dw = [row(c) - mine[c] for c in range(6)]
            radius_sq = (dx * dx + dy * dy) + (dz * dz + SOFTEN_SQ)
            root = lax.rsqrt(radius_sq)
            inverse = root * root
            weight = (row(6) * root) * inverse
            radial = (dx * du + dy * dv + dz * dw) * inverse
            wx, wy, wz = weight * dx, weight * dy, weight * dz
            new = (wx, wy, wz, weight * du, weight * dv, weight * dw, radial * wx, radial * wy, radial * wz)
            return tuple(s + n for s, n in zip(sums_here, new))

        zero = jnp.zeros((8, LANES), jnp.float32)
        got = lax.fori_loop(0, n_field, one_chunk, (zero,) * 9, unroll=UNROLL)
        for c in range(3):
            sums[c, at, :] = got[c]
            sums[3 + c, at, :] = got[3 + c] - 3.0 * got[6 + c]
        return carry

    lax.fori_loop(0, (total + 7) // 8, one_block, 0)
    folded = jnp.zeros((8, WIDE), jnp.float32)
    for c in range(6):
        ones = (row_iota((8, LANES)) == c).astype(jnp.bfloat16)
        row = jnp.zeros((8, WIDE), jnp.float32)
        for part in exact_parts(sums[c]):
            row = row + lax.dot_general(ones, part, (((1,), (1,)), ((), ())), preferred_element_type=jnp.float32)
        row = jnp.where(row_iota((8, WIDE)) == c, row, 0.0)
        folded = folded + (pltpu.roll(row, SLOTS * c, 1) if c else row)
    lane = lane_iota((8, LANES))
    owned = own_rows((8, LANES))
    copy.wait()
    for k in range(n_line):
        moved = pltpu.roll(folded, WIDE - known[0, k], 1) if k else folded
        kept = jnp.where(owned & (lane % SLOTS < known[1, k]), moved, 0.0)
        packed = jnp.sum(kept, axis=0, keepdims=True)
        for j, member in enumerate(order):
            if member // 2 == k:
                out[j] = packed


def correct_kernel(table, parts, pos, vel, acc, jerk, new_pos, new_vel, new_acc, new_jerk):
    force = parts[0]
    for k in range(1, parts.shape[0]):
        force = force + parts[k]
    shape = (8, LANES)
    spread = jnp.where(own_rows(shape), jnp.broadcast_to(force, shape), 0.0)
    spread = jnp.where((row_iota(shape) == 6) & own_rows(shape), 1.0, spread)
    placed = jnp.zeros((8, table.shape[1]), jnp.float32)
    for part in exact_parts(spread):
        placed = placed + jnp.dot(part, table[...], preferred_element_type=jnp.float32)
    hit = jnp.broadcast_to(placed[6:7], (3, placed.shape[1])) > 0.5
    acc_one, jerk_one = placed[0:3], placed[3:6]
    pos_zero, vel_zero, acc_zero, jerk_zero = pos[...], vel[...], acc[...], jerk[...]
    twelfth = STEP_TIME * STEP_TIME / 12.0
    vel_one = vel_zero + (acc_zero + acc_one) * (STEP_TIME / 2.0) + (jerk_zero - jerk_one) * twelfth
    pos_one = pos_zero + (vel_zero + vel_one) * (STEP_TIME / 2.0) + (acc_zero - acc_one) * twelfth
    new_pos[...] = jnp.where(hit, pos_one, pos_zero)
    new_vel[...] = jnp.where(hit, vel_one, vel_zero)
    new_acc[...] = jnp.where(hit, acc_one, acc_zero)
    new_jerk[...] = jnp.where(hit, jerk_one, jerk_zero)


def f32(*shape):
    return jax.ShapeDtypeStruct(shape, jnp.float32)


VMEM = pl.BlockSpec(memory_space=pltpu.VMEM)
HBM = pl.BlockSpec(memory_space=pltpu.HBM)


def shards(star_pos, star_vel, star_acc, star_jerk, masses, act_index, act_count):
    n_field = lax.axis_size(FIELD_AXES)
    n_line = lax.axis_size(ACT_AXIS)
    state = (star_pos, star_vel, star_acc, star_jerk)
    width = star_pos.shape[1]

    def line():
        y, x, z = line_base()
        return x * lax.axis_size(Z) + z, lax.axis_size(X) * lax.axis_size(Z)

    given = (*state, masses[None, :], act_index, act_count)
    call = dict(compiler_params=pltpu.CompilerParams(vmem_limit_bytes=LIMIT))
    field, act, meta, table = pl.pallas_call(
        lambda *refs: prepare_kernel(line, *refs),
        out_shape=(
            pltpu.VMEM((n_field, 7, LANES), jnp.float32),
            pltpu.VMEM((1, LANES), jnp.float32),
            pltpu.VMEM((8, LANES), jnp.int32),
            pltpu.VMEM((LANES, width), jnp.bfloat16),
        ),
        in_specs=[HBM] * 7,
        out_specs=(VMEM,) * 4,
        scratch_shapes=[pltpu.VMEM((3, width), jnp.float32)] * 4
        + [
            pltpu.VMEM((1, width), jnp.float32),
            pltpu.VMEM((1, SLOTS), jnp.int32),
            pltpu.SMEM(act_count.shape, jnp.int32),
            pltpu.VMEM((8, width), jnp.float32),
            pltpu.VMEM((8, LANES), jnp.int32),
            pltpu.SemaphoreType.DMA((7,)),
        ],
        name="prepare",
        **call,
    )(*[pltpu.with_memory_space_constraint(a, pltpu.HBM) for a in given])
    field = lax.all_to_all(field, FIELD_AXES, 0, 0, tiled=True)
    act = lax.all_gather(act, ACT_AXIS)
    active = pl.pallas_call(
        spread_kernel,
        out_shape=pltpu.VMEM((6, WIDE + SLOTS, LANES), jnp.float32),
        in_specs=[VMEM] * 2,
        out_specs=VMEM,
        scratch_shapes=[pltpu.VMEM((8, LANES), jnp.float32)],
        name="spread",
        **call,
    )(meta, act)
    order = [2 * ((j // 2 + n_line // 2) % n_line) + 1 - j % 2 for j in range(2 * n_line)]
    parts = pl.pallas_call(
        lambda *refs: forces_kernel(order, *refs),
        out_shape=pltpu.VMEM((2 * n_line, 1, LANES), jnp.float32),
        in_specs=[VMEM] * 3,
        out_specs=VMEM,
        scratch_shapes=[
            pltpu.VMEM((6, WIDE, LANES), jnp.float32),
            pltpu.SMEM((8, LANES), jnp.int32),
            pltpu.SemaphoreType.DMA(()),
        ],
        name="forces",
        **call,
    )(meta, field, active)
    parts = lax.all_to_all(parts, (ACT_AXIS, REP), 0, 0, axis_index_groups=[order], tiled=True)
    return pl.pallas_call(
        correct_kernel,
        out_shape=tuple(f32(3, width) for _ in range(4)),
        in_specs=[VMEM] * 6,
        out_specs=(VMEM,) * 4,
        name="correct",
        **call,
    )(table, parts, *state)


def solution(mesh):
    finer = Mesh(mesh.devices.reshape(8, 4, 12, mesh.shape["rep"]), (Y, X, Z, REP))
    placed = (P(None, BLK), P(None, BLK), P(None, BLK), P(None, BLK), P(BLK), P(BLK, None), P())
    return jax.shard_map(
        shards,
        mesh=finer,
        in_specs=placed,
        out_specs=(P(None, BLK), P(None, BLK), P(None, BLK), P(None, BLK)),
        check_vma=False,
    )
```
